32 devices in a mesh: face: 4 (over y, x), tile: 8 (over z, core).
Axes of the slice: x: 2, y: 2, z: 4, core: 2. Of those that a mesh axis runs over, the one named last changes fastest.
Arguments:
- atmos_state: bfloat16 [128, 512, 1024], P(None, 'face', 'tile'), may hold values from -6 to 6
- ocean_state: bfloat16 [64, 512, 1024], P(None, 'face', 'tile'), may hold values from -6 to 6
- land_mask: int32 [512, 32], P('face', 'tile'), may hold values 0 or 1
- face_turns: int32 [4, 8], P('face', 'tile'), may hold values from 0 to 3
- block_target: int32 [4096, 1], P(('face', 'tile')), may hold values from 0 to 31; in each aligned block of 128 rows (0 to 127, 128 to 255, ...) at most 8 rows name the same one
- block_patch: int32 [4096, 1], P(('face', 'tile')), may hold values from 0 to 127
- block_weight: float32 [4096, 1], P(('face', 'tile')), may hold values from 0.25 to 1
- atmos_w1: bfloat16 [9, 128, 144], replicated, may hold values from -0.15625 to 0.15625
- atmos_w2: bfloat16 [9, 128, 128], replicated, may hold values from -0.1875 to 0.1875
- ocean_w1: bfloat16 [9, 64, 80], replicated, may hold values from -0.21875 to 0.21875
- ocean_w2: bfloat16 [9, 64, 64], replicated, may hold values from -0.25 to 0.25
Outputs:
- atmos_out: bfloat16 [128, 512, 1024], P(None, 'face', 'tile')
- ocean_out: bfloat16 [64, 512, 1024], P(None, 'face', 'tile')
The draws below stay inside these ranges and needn't reach their ends.
Inputs may be any that keep to these rules, and one draw needn't show every extreme that they name: `block_target`: among the 128 blocks of one device, at most 8 have the same target, and in every draw some device has exactly 8 blocks with one target.
All inputs are finite; a program needn't handle non-finite values. No bound on the sum of `land_mask` on one device may be relied on, other than what follows from the above.
Results may differ from the reference program's by a relative error of at most 0.001.
The reference program's roundings to bfloat16 on the way (of `common`, `masked_ocean`, `weights`, `sea_surface`, `forcing`, `hidden_atmos`, `atmos_common_out` and `hidden_ocean`) count: a program that leaves them out, or rounds other values in their place, can miss the bound.
Values may be sent and summed in bfloat16 or wider, within the bound.
No kernel may reach another device: no remote copies, remote signals or barrier semaphores. Data moves between devices by JAX's collectives and lax.ppermute only.
A program may use at most 192 MiB of HBM per device.

```python
import math
from functools import partial
import jax
import jax.numpy as jnp
import numpy as np
from jax import lax

CA = 128
CO = 64
CS = 16
CF = 16
S = 128
OH = 128
NAY = 512
NAX = 1024
NOY = 512
NOX = 1024
BLOCKS = 4096
CAP = 8
N_FACE = 4
N_TILE = 8
DEVICES = 32


def set_ends(values, rng, low, largest):
    shape = values.shape
    index_at = [jax.random.randint(jax.random.fold_in(rng, axis), (), 0, shape[axis]) for axis in range(len(shape))]
    values = values.at[tuple(index_at)].set(low)
    longest = shape.index(max(shape))
    index_at[longest] = (index_at[longest] + 1) % shape[longest]
    return values.at[tuple(index_at)].set(largest)


def levels(key, shape, split, least, top_value):
    loudness = 1.0
    for axis_at, blocks in split:
        steps = jax.random.uniform(jax.random.fold_in(jax.random.fold_in(key, 6), axis_at), (blocks,), jnp.float32, least / len(split), top_value / len(split))
        loudness = loudness * jnp.repeat(jnp.exp(steps), shape[axis_at] // blocks).reshape((-1,) + (1,) * (len(shape) - 1 - axis_at))
    return loudness


def assign_block(own_key, own, number, rows, number_of, top, most, slope):
    order = jax.random.permutation(own_key, number_of)
    heavy_load, usual = load_shares(number_of, rows * top, most, slope, True), load_shares(number_of, rows * top, most, slope, False)
    places = jnp.arange(number_of)

    def named(tallies, turn):
        used = int((tallies > 0).sum())
        fixed = max(1, used // 4)
        moved = fixed + (places - fixed + turn * (used - fixed)) % max(1, number_of - fixed)
        return jnp.zeros((number_of,), jnp.int32).at[order[jnp.where(places < fixed, places, moved)]].set(jnp.asarray(tallies, jnp.int32))

    tallies = jnp.where(number % 4 == 0, named(heavy_load, number // 4), named(usual, number - number // 4 - 1))
    mixed = jax.random.permutation(jax.random.fold_in(own, 3), number_of)
    donor, taker = mixed[0:number_of // 2 * 2:2], mixed[1:number_of // 2 * 2:2]
    room = jnp.minimum(tallies[donor] - 1, most - tallies[taker]) // 2
    room = jnp.where((donor == order[0]) | (taker == order[0]) | (tallies[taker] == 0), 0, jnp.maximum(room, 0))
    moved = jax.random.randint(jax.random.fold_in(own, 4), (number_of // 2,), 0, 1 << 20) % (room + 1)
    tallies = tallies.at[donor].add(-moved).at[taker].add(moved)
    labels = jnp.searchsorted(jnp.cumsum(tallies), jnp.arange(rows * top), side="right").astype(jnp.int32)
    grid = labels.reshape(top, rows).T
    grid = grid[jax.random.permutation(jax.random.fold_in(own, 1), rows)]
    turn = jax.random.randint(jax.random.fold_in(own, 2), (rows, 1), 0, top)
    return jnp.take_along_axis(grid, (jnp.arange(top)[None, :] + turn) % top, axis=1)


def load_shares(amount, total, most, slope, full):
    loads = [(1 << 20) // math.isqrt(rank ** slope) + 1 for rank in range(1, amount + 1)]
    largest = most if full else min(most, max(-(-total // amount), total * loads[0] // sum(loads)))
    least = 1 if total - largest >= amount - 1 else 0
    counts, surplus = [largest] + [least] * (amount - 1), total - largest - least * (amount - 1)
    while surplus > 0:
        movable = [i for i in range(1, amount) if counts[i] < largest] or [i for i in range(1, amount) if counts[i] < most]
        whole, budget = sum([loads[i] for i in movable]), surplus
        for i in movable:
            extra = min(most - counts[i], max(1, budget * loads[i] // whole), surplus)
            counts[i] = counts[i] + extra
            surplus = surplus - extra
    return np.array(counts)


def scatter_about(rng, shape, spread, reach, pieces=(), held_as=jnp.bfloat16):
    values = spread * jax.random.normal(rng, shape, jnp.float32)
    if pieces:
        values = values * levels(rng, shape, pieces, -0.22, 0.18)
    return jnp.clip(values, -reach, reach).astype(held_as)


def setup_inputs(seed: int = 0) -> dict:
    key_list = jax.random.split(jax.random.key(seed), 12)
    atmos_state = scatter_about(key_list[0], (CA, NAY, NAX), 1.0, 6.0, ((1, 4), (2, 8)))
    ocean_state = scatter_about(key_list[1], (CO, NOY, NOX), 1.0, 6.0, ((1, 4), (2, 8)))
    land_mask = set_ends((jax.random.randint(key_list[2], (NOY, NOX // 32), 0, 4) < 3).astype(jnp.int32), jax.random.fold_in(key_list[2], 1), 0, 1)
    face_turns = set_ends(jax.random.randint(key_list[3], (N_FACE, N_TILE), 0, 4), jax.random.fold_in(key_list[3], 1), 0, 3).astype(jnp.int32)
    block_target_keys = jax.random.split(jax.random.fold_in(key_list[4], 1), BLOCKS // OH)
    block_target_turns = jax.random.permutation(jax.random.fold_in(key_list[4], 3), BLOCKS // OH)
    block_target = jax.vmap(lambda own, number: assign_block(jax.random.fold_in(key_list[4], 2), own, number, OH, DEVICES, 1, CAP, 2))(block_target_keys, block_target_turns).reshape((BLOCKS, 1))
    block_patch = set_ends(jax.random.randint(key_list[5], (BLOCKS, 1), 0, S), jax.random.fold_in(key_list[5], 1), 0, S - 1).astype(jnp.int32)
    block_weight = jnp.clip(jnp.exp(math.log(1.0) - 1.3862944 * jax.random.uniform(key_list[6], (BLOCKS, 1), jnp.float32) ** levels(key_list[6], (BLOCKS, 1), ((0, 32),), -0.2, 0.2)), 0.25, 1.0)
    atmos_w1 = scatter_about(key_list[7], (9, CA, CA + CS), (9 * (CA + CS)) ** -0.5, 0.15625)
    atmos_w2 = scatter_about(key_list[8], (9, CA, CA), (9 * CA) ** -0.5, 0.1875)
    ocean_w1 = scatter_about(key_list[9], (9, CO, CO + CF), (9 * (CO + CF)) ** -0.5, 0.21875)
    ocean_w2 = scatter_about(key_list[10], (9, CO, CO), (9 * CO) ** -0.5, 0.25)
    return {"atmos_state": atmos_state, "ocean_state": ocean_state, "land_mask": land_mask, "face_turns": face_turns, "block_target": block_target, "block_patch": block_patch, "block_weight": block_weight, "atmos_w1": atmos_w1, "atmos_w2": atmos_w2, "ocean_w1": ocean_w1, "ocean_w2": ocean_w2}


def turn_tile(tile_data, quarter_turns):
    return jnp.rot90(tile_data, quarter_turns, axes=(1, 2))


def turn_all(tiles, turns, sign):
    branches = [partial(turn_tile, quarter_turns=sign * quarter) for quarter in range(4)]

    def apply_turn(packed):
        return lax.switch(packed[1], branches, packed[0])

    return lax.map(apply_turn, (tiles, turns))


def to_tiles(values):
    channels = values.shape[0]
    shaped = values.reshape(channels, N_FACE, S, N_TILE, S).transpose(1, 3, 0, 2, 4)
    return shaped.reshape(N_FACE * N_TILE, channels, S, S)


def from_tiles(tiles):
    channels = tiles.shape[1]
    shaped = tiles.reshape(N_FACE, N_TILE, channels, S, S).transpose(2, 0, 3, 1, 4)
    return shaped.reshape(channels, N_FACE * S, N_TILE * S)


def convolve(padded, weight, block_rows, finish):
    col_count = padded.shape[2] - 2
    block_count = (padded.shape[1] - 2) // block_rows
    kernel = weight.astype(jnp.float32)

    def one_block(block_id):
        part = lax.dynamic_slice_in_dim(padded, block_id * block_rows, block_rows + 2, 1).astype(jnp.float32)
        summed = jnp.zeros((kernel.shape[1], block_rows, col_count), jnp.float32)
        for row_shift in range(3):
            for col_shift in range(3):
                window = part[:, row_shift:row_shift + block_rows, col_shift:col_shift + col_count]
                summed = summed + jnp.einsum("oc,cyx->oyx", kernel[row_shift * 3 + col_shift], window)
        return finish(summed, block_id)

    result = lax.map(one_block, jnp.arange(block_count, dtype=jnp.int32))
    return result.transpose(1, 0, 2, 3).reshape(result.shape[1], block_count * block_rows, col_count)


def wrap_pad(values):
    return jnp.pad(values, ((0, 0), (1, 1), (1, 1)), mode="wrap")


def fold_pad(values):
    wrapped = jnp.pad(values, ((0, 0), (0, 0), (1, 1)), mode="wrap")
    north_row = wrapped[:, -1:, ::-1]
    south_row = jnp.zeros_like(north_row)
    return jnp.concatenate([south_row, wrapped, north_row], axis=1)


def activate(summed, block_id):
    return jax.nn.gelu(summed, approximate=True).astype(jnp.bfloat16)


def reference(atmos_state, ocean_state, land_mask, face_turns, block_target, block_patch, block_weight, atmos_w1, atmos_w2, ocean_w1, ocean_w2):
    tile_total = N_FACE * N_TILE
    turns = face_turns.reshape(-1)
    common = from_tiles(turn_all(to_tiles(atmos_state), turns, -1))
    mask_cells = jnp.repeat(land_mask, 32, axis=1).astype(jnp.bfloat16)
    masked_ocean = ocean_state * mask_cells[None]
    ocean_blocks = masked_ocean[:CS].reshape(CS, N_FACE, OH, N_TILE, S).transpose(1, 3, 2, 0, 4)
    ocean_blocks = ocean_blocks.reshape(tile_total * OH, CS * S).astype(jnp.float32)
    rounded = lax.optimization_barrier(block_weight[:, 0].astype(jnp.bfloat16))
    weights = rounded.astype(jnp.float32)
    patch_ids = (block_target[:, 0] * S + block_patch[:, 0]).astype(jnp.int32)
    numerator = jax.ops.segment_sum(ocean_blocks * weights[:, None], patch_ids, num_segments=tile_total * S)
    denominator = jax.ops.segment_sum(weights, patch_ids, num_segments=tile_total * S)
    sea_rows = (numerator / jnp.maximum(denominator, 1.0)[:, None]).astype(jnp.bfloat16)
    sea_surface = sea_rows.reshape(N_FACE, N_TILE, S, CS, S).transpose(3, 0, 2, 1, 4).reshape(CS, N_FACE * S, N_TILE * S)
    atmos_rows = common[:CF].reshape(CF, N_FACE, S, N_TILE, S).transpose(1, 3, 2, 0, 4).reshape(tile_total * S, CF * S)
    facing = jnp.take(atmos_rows, patch_ids, axis=0)
    forcing = facing.reshape(N_FACE, N_TILE, OH, CF, S).transpose(3, 0, 2, 1, 4).reshape(CF, N_FACE * OH, N_TILE * S)

    atmos_in = jnp.concatenate([common, sea_surface], axis=0)
    hidden_atmos = convolve(wrap_pad(atmos_in), atmos_w1, S, activate)

    def finish_atmos(summed, block_id):
        base = lax.dynamic_slice_in_dim(common, block_id * S, S, 1).astype(jnp.float32)
        return (base + summed).astype(jnp.bfloat16)

    atmos_common_out = convolve(wrap_pad(hidden_atmos), atmos_w2, S, finish_atmos)
    atmos_out = from_tiles(turn_all(to_tiles(atmos_common_out), turns, 1))

    ocean_in = jnp.concatenate([masked_ocean, forcing], axis=0)
    hidden_ocean = convolve(fold_pad(ocean_in), ocean_w1, OH, activate)
    mask_float = mask_cells.astype(jnp.float32)

    def finish_ocean(summed, block_id):
        base = lax.dynamic_slice_in_dim(masked_ocean, block_id * OH, OH, 1).astype(jnp.float32)
        gate = lax.dynamic_slice_in_dim(mask_float, block_id * OH, OH, 0)
        return (gate[None] * (base + summed)).astype(jnp.bfloat16)

    ocean_out = convolve(fold_pad(hidden_ocean), ocean_w2, OH, finish_ocean)
    return atmos_out, ocean_out
```

```python
from functools import partial

import jax
import jax.numpy as jnp
import numpy as np
from jax import lax
from jax.experimental import pallas as pl
from jax.experimental.pallas import tpu as pltpu
from jax.sharding import PartitionSpec as P

CS = 16
CF = 16
RUN = 32
F32 = jnp.float32
BF16 = jnp.bfloat16
VM = pl.BlockSpec(memory_space=pltpu.VMEM)
SM = pl.BlockSpec(memory_space=pltpu.SMEM)
SMALL = pltpu.CompilerParams(vmem_limit_bytes=16 << 20)


def iota(shape, axis):
    return lax.broadcasted_iota(jnp.int32, shape, axis)


def dot(a, b, dims=((1,), (0,))):
    return lax.dot_general(a, b, (dims, ((), ())), preferred_element_type=F32)


def reverser(size, flip):
    rows, cols = iota((size, size), 0), iota((size, size), 1)
    wanted = jnp.where(flip, size - 1 - rows, rows)
    return jnp.where(cols == wanted, 1.0, 0.0).astype(BF16)


def cell_mask(land, cols):
    runs, rows = land.shape
    parts = [
        jnp.broadcast_to(land[run : run + 1, :].astype(F32), (cols // runs, rows))
        for run in range(runs)
    ]
    return jnp.concatenate(parts, axis=0).T


def across(row):
    return jnp.broadcast_to(row.astype(F32), (row.shape[1],) * 2)


def pack_kernel(capacity, surface, land, target, weight, patch, out):
    rows, cols = surface.shape[1], surface.shape[2]
    slots = out.shape[0]
    first, second = iota((rows, rows), 0), iota((rows, rows), 1)
    targets = across(target[...])
    same = (targets.T == targets) & (first < second)
    rank = jnp.sum(jnp.where(same, 1.0, 0.0), axis=0, keepdims=True)
    slot = (targets[0:1, :] * capacity + rank).astype(jnp.int32)
    packer = jnp.where(iota((slots, rows), 0) == slot, 1.0, 0.0).astype(BF16)
    mask = cell_mask(land[...], cols).astype(BF16)
    for c in range(CS):
        out[:, c * cols : (c + 1) * cols] = dot(packer, surface[c] * mask).astype(BF16)
    lanes = iota((rows, rows), 1)
    described = jnp.where(
        lanes == 0, across(weight[...]).T, jnp.where(lanes == 1, across(patch[...]).T, 0.0)
    )
    out[:, CS * cols :] = dot(packer, described.astype(BF16)).astype(BF16)


def common_kernel(turn, surface, out):
    side = surface.shape[1]
    k = turn[0, 0]
    flip_rows = reverser(side, k >= 2)
    flip_cols = reverser(side, (k == 1) | (k == 2))
    odd = (k % 2) == 1
    for c in range(CF):
        tile = surface[c].astype(F32)
        tile = jnp.where(odd, tile.T, tile).astype(BF16)
        tile = dot(tile, flip_cols).astype(BF16)
        out[:, c * side : (c + 1) * side] = dot(flip_rows, tile).astype(BF16)


def return_kernel(meta, rows, out):
    slots, side = meta.shape
    patch = meta[:, 1:2].astype(F32).astype(jnp.int32)
    select = jnp.where(iota((slots, side), 1) == patch, 1.0, 0.0).astype(BF16)
    for c in range(CF):
        part = slice(c * side, (c + 1) * side)
        out[:, part] = dot(select, rows[:, part]).astype(BF16)


def turn_edges(k, edges, size):
    width = edges[0].shape[1]
    rows, cols = iota((width, width), 0), iota((width, width), 1)
    flip = jnp.where(rows + cols == size - 1, 1.0, 0.0).astype(BF16)
    top, bottom, left, right = edges
    top_r, bottom_r, left_r, right_r = [dot(value.astype(BF16), flip) for value in edges]

    def chosen(*options):
        value = options[3]
        for number in range(3):
            value = jnp.where(k == number, options[number], value)
        return value

    return (
        chosen(top, left_r, bottom_r, right),
        chosen(bottom, right_r, top_r, left),
        chosen(left, bottom, right_r, top_r),
        chosen(right, top, left_r, bottom_r),
    )


def column_edges(ref):
    count, channels, cols = ref.shape
    lanes = iota((channels, count), 1)

    def step(y, carry):
        row = ref[y].astype(F32)
        return (
            jnp.where(lanes == y, row[:, 0:1], carry[0]),
            jnp.where(lanes == y, row[:, cols - 1 :], carry[1]),
        )

    zero = jnp.zeros((channels, count), F32)
    return lax.fori_loop(0, count, step, (zero, zero), unroll=16)


def all_edges(ref):
    last = ref.shape[0] - 1
    return (ref[0].astype(F32), ref[last].astype(F32), *column_edges(ref))


def early_kernel(turn, state, ocean, *outs):
    atmos = turn_edges(turn[0, 0], all_edges(state), state.shape[2])
    sea = all_edges(ocean)
    for out, above, below in zip(outs, atmos, sea):
        out[...] = jnp.concatenate([above, below], axis=0).astype(BF16)


def sea_kernel(turn, incoming, out, *edges):
    side = out.shape[0]
    slots = incoming.shape[0]
    k = turn[0, 0]
    flip_x = reverser(side, (k == 1) | (k == 2))
    meta = incoming[:, CS * side :].astype(F32)

    def placed(patch):
        patch = patch.astype(jnp.int32)
        return jnp.where(k >= 2, side - 1 - patch, patch)

    @pl.when((k % 2) == 0)
    def _():
        turned = meta.T
        spread = jnp.where(
            iota((side, slots), 0) == placed(turned[1:2, :]), turned[0:1, :], 0.0
        )
        scale = jnp.maximum(jnp.sum(spread, axis=1, keepdims=True), 1.0)
        spread = spread.astype(BF16)
        for c in range(CS):
            part = dot(incoming[:, c * side : (c + 1) * side], flip_x).astype(BF16)
            value = dot(spread, part) / scale
            out[:, c, :] = value.astype(BF16).astype(F32)

    @pl.when((k % 2) == 1)
    def _():
        spread = jnp.where(
            iota((slots, side), 1) == placed(meta[:, 1:2]), meta[:, 0:1], 0.0
        )
        scale = jnp.maximum(jnp.sum(spread, axis=0, keepdims=True), 1.0)
        spread = spread.astype(BF16)
        for c in range(CS):
            part = dot(incoming[:, c * side : (c + 1) * side], flip_x)
            value = dot(part.T.astype(BF16), spread) / scale
            out[:, c, :] = value.astype(BF16).astype(F32)

    for edge, value in zip(edges, turn_edges(k, all_edges(out), side)):
        edge[...] = value.astype(BF16)


def force_kernel(capacity, target, returned, out, *edges):
    rows, cols = out.shape[0], out.shape[2]
    slots = returned.shape[0]
    first, second = iota((rows, rows), 0), iota((rows, rows), 1)
    targets = across(target[...])
    same = (targets.T == targets) & (second < first)
    rank = jnp.sum(jnp.where(same, 1.0, 0.0), axis=1, keepdims=True)
    slot = (targets.T[:, 0:1] * capacity + rank).astype(jnp.int32)
    pick = jnp.where(iota((rows, slots), 1) == slot, 1.0, 0.0).astype(BF16)
    for c in range(CF):
        out[:, c, :] = dot(pick, returned[:, c * cols : (c + 1) * cols])
    for edge, value in zip(edges, all_edges(out)):
        edge[...] = value.astype(BF16)


def widened(value):
    return jnp.concatenate([value, jnp.zeros_like(value)], axis=1)


def framed(before, value, after):
    cols = value.shape[1]
    lanes = iota((value.shape[0], 2 * cols), 1)
    moved = pltpu.roll(widened(value), 1, 1)
    return jnp.where(lanes == 0, before, jnp.where(lanes == cols + 1, after, moved))


def side_kernel(start, place, above, below, fold, left, right, *outs):
    to_left, to_right, above_out, below_out = outs
    over, under = above[...].astype(F32), below[...].astype(F32)
    if fold is not None:
        channels, cols = over.shape
        ocean = iota((channels, cols), 0) >= start
        over = jnp.where(ocean & (place[0] == 0), 0.0, over)
        flip = reverser(cols, True)
        back = dot(fold[...], flip)
        if start:
            back = jnp.concatenate([jnp.zeros((start, cols), F32), back], axis=0)
        under = jnp.where(ocean & (place[0] == 1), back, under)
    above_out[...] = over.astype(BF16)
    below_out[...] = under.astype(BF16)
    cols = over.shape[1]
    to_left[...] = framed(over[:, :1], left[...].astype(F32), under[:, :1]).astype(BF16)
    to_right[...] = framed(
        over[:, cols - 1 :], right[...].astype(F32), under[:, cols - 1 :]
    ).astype(BF16)


def halo_kernel(spans, turned, turn, *refs):
    ends, left, right = refs[-3:]
    pieces = []
    for number, (low, high) in enumerate(spans):
        above, below, from_left, from_right = [
            ref[low:high, :].astype(F32) for ref in refs[4 * number : 4 * number + 4]
        ]
        last = above.shape[1] + 1
        pieces.append(
            (
                framed(from_left[:, :1], above, from_right[:, :1]),
                framed(from_left[:, last : last + 1], below, from_right[:, last : last + 1]),
                from_left,
                from_right,
            )
        )
    halo = [jnp.concatenate(part, axis=0) if len(part) > 1 else part[0] for part in zip(*pieces)]
    if turned:
        halo = turn_edges(lax.rem(4 - turn[0, 0], 4), halo, left.shape[1] + 2)
    ends[0], ends[1] = halo[0], halo[1]
    cols = left.shape[1]
    width = 2 * cols
    left[...] = pltpu.roll(halo[2], width - 1, 1)[:, :cols]
    right[...] = pltpu.roll(halo[3], width - 1, 1)[:, :cols]


def conv_kernel(parts, mode, *refs):
    refs = list(refs)
    turn = refs.pop(0)
    sources = [refs.pop(0) for _ in range(parts)]
    ends, left, right, taps = [refs.pop(0) for _ in range(4)]
    base = refs.pop(0) if mode in ("add", "masked") else None
    mask = refs.pop(0) if mode == "masked" else None
    out = refs.pop(0)
    gelu = mode in ("turned", "plain")
    edges = [refs.pop(0) for _ in range(4)] if gelu else None
    stacked, sums, early, late = refs[:4]
    edge_left, edge_right = refs[4:] if gelu else (None, None)
    rows, outputs, cols = out.shape
    channels = ends.shape[1]
    lanes = iota((channels, cols), 1)
    out_lanes = iota((outputs, cols), 1)

    def place(slot, half, shifted):
        for b, value in enumerate(shifted):
            stacked[slot, b * channels : (b + 1) * channels, half * cols : (half + 1) * cols] = (
                value.astype(BF16)
            )

    def inner(slot, half, y):
        row = [source[y].astype(F32) for source in sources]
        row = row[0] if parts == 1 else jnp.concatenate(row, axis=0)
        before = pltpu.roll(left[...], lax.rem(cols - y, cols), 1)
        after = pltpu.roll(right[...], cols - 1 - y, 1)
        place(
            slot,
            half,
            (
                jnp.where(lanes == 0, before, pltpu.roll(row, 1, 1)),
                row,
                jnp.where(lanes == cols - 1, after, pltpu.roll(row, cols - 1, 1)),
            ),
        )

    def end(slot, half, which):
        row = ends[which]
        place(slot, half, [row[:, b : b + cols] for b in range(3)])

    def emit(y, value):
        if gelu:
            value = jax.nn.gelu(value, approximate=True).astype(BF16)
            out[y] = value
            value = value.astype(F32)
            edge_left[...] = jnp.where(out_lanes == y, value[:, 0:1], edge_left[...])
            edge_right[...] = jnp.where(out_lanes == y, value[:, cols - 1 :], edge_right[...])
        else:
            value = base[y].astype(F32) + value
            if mode == "masked":
                value = value * mask[y]
            out[y] = value.astype(BF16)

    def product(slot):
        sums[slot] = dot(taps[...], stacked[slot])

    def tap(slot, a, half):
        return sums[slot, a * outputs : (a + 1) * outputs, half * cols : (half + 1) * cols]

    def carry(slot):
        early[...] = tap(slot, 0, 0) + tap(slot, 1, 1)
        late[...] = tap(slot, 0, 1)

    def finish(slot, j):
        emit(2 * j - 2, early[...] + tap(slot, 2, 0))
        emit(2 * j - 1, late[...] + tap(slot, 1, 0) + tap(slot, 2, 1))
        carry(slot)

    def load(slot, j):
        inner(slot, 0, 2 * j - 1)
        inner(slot, 1, 2 * j)

    spare = stacked.shape[1] - 3 * channels
    if spare:
        stacked[:, 3 * channels :, :] = jnp.zeros((stacked.shape[0], spare, 2 * cols), BF16)
    if gelu:
        edge_left[...] = jnp.zeros(edge_left.shape, F32)
        edge_right[...] = jnp.zeros(edge_right.shape, F32)
    pairs = rows // 2
    end(0, 0, 0)
    inner(0, 1, 0)
    product(0)
    load(1, 1)
    carry(0)
    product(1)
    load(0, 2)

    def step(i, _):
        j = 2 * i + 2
        product(0)
        finish(1, j - 1)
        load(1, j + 1)
        product(1)
        finish(0, j)
        load(0, j + 2)
        return 0

    lax.fori_loop(0, pairs // 2 - 2, step, 0)
    product(0)
    finish(1, pairs - 3)
    load(1, pairs - 1)
    product(1)
    finish(0, pairs - 2)
    inner(0, 0, rows - 1)
    end(0, 1, 1)
    product(0)
    finish(1, pairs - 1)
    finish(0, pairs)
    if gelu:
        found = (
            out[0].astype(F32),
            out[rows - 1].astype(F32),
            edge_left[...],
            edge_right[...],
        )
        if mode == "turned":
            found = turn_edges(turn[0, 0], found, cols)
        for edge, value in zip(edges, found):
            edge[...] = value.astype(BF16)


def convolve(turn, sources, halo, taps, mode, base=None, mask=None):
    rows, _, cols = sources[0].shape
    outputs = taps.shape[0] // 3
    operands = [turn, *sources, *halo, taps]
    operands += [value for value in (base, mask) if value is not None]
    shapes = [jax.ShapeDtypeStruct((rows, outputs, cols), BF16)]
    scratch = [
        pltpu.VMEM((2, taps.shape[1], 2 * cols), BF16),
        pltpu.VMEM((2, taps.shape[0], 2 * cols), F32),
        pltpu.VMEM((outputs, cols), F32),
        pltpu.VMEM((outputs, cols), F32),
    ]
    if base is None:
        shapes += [jax.ShapeDtypeStruct((outputs, cols), BF16)] * 4
        scratch += [pltpu.VMEM((outputs, cols), F32)] * 2
    result = pl.pallas_call(
        partial(conv_kernel, len(sources), mode),
        out_shape=shapes,
        in_specs=[SM] + [VM] * (len(operands) - 1),
        out_specs=[VM] * len(shapes),
        scratch_shapes=scratch,
        compiler_params=SMALL,
    )(*operands)
    return (result[0], result[1:]) if base is None else result[0]


def shifted(value, axis, distance):
    count = lax.axis_size(axis)
    return lax.ppermute(value, axis, [(i, (i + distance) % count) for i in range(count)])


def exchanged(edges, place, start=None):
    top, bottom, left, right = edges
    channels, cols = top.shape
    above = shifted(bottom, "face", 1)
    below = shifted(top, "face", -1)
    operands = [above, below]
    if start is not None:
        faces, tiles = lax.axis_size("face"), lax.axis_size("tile")
        north = (faces - 1) * tiles
        operands.append(
            lax.ppermute(
                bottom[start:],
                ("face", "tile"),
                [(north + t, north + tiles - 1 - t) for t in range(tiles)],
            )
        )
    operands += [left, right]
    kernel = partial(side_kernel, start)
    if start is None:

        def kernel(place, above, below, left, right, *outs):
            side_kernel(None, place, above, below, None, left, right, *outs)

    to_left, to_right, above, below = pl.pallas_call(
        kernel,
        out_shape=[jax.ShapeDtypeStruct((channels, 2 * cols), BF16)] * 2
        + [jax.ShapeDtypeStruct((channels, cols), BF16)] * 2,
        in_specs=[SM] + [VM] * len(operands),
        out_specs=[VM] * 4,
        compiler_params=SMALL,
    )(place, *operands)
    return above, below, shifted(to_right, "tile", 1), shifted(to_left, "tile", -1)


def halo_of(turn, spans, turned, *pieces):
    channels = sum(high - low for low, high in spans)
    cols = pieces[0][0].shape[1]
    operands = [value for piece in pieces for value in piece]
    return pl.pallas_call(
        partial(halo_kernel, spans, turned),
        out_shape=[jax.ShapeDtypeStruct((2, channels, 2 * cols), F32)]
        + [jax.ShapeDtypeStruct((channels, cols), F32)] * 2,
        in_specs=[SM] + [VM] * len(operands),
        out_specs=[VM] * 3,
        compiler_params=SMALL,
    )(turn, *operands)


def stack_taps(weight):
    _, outputs, channels = weight.shape
    taps = weight.reshape(3, 3, outputs, channels).transpose(0, 2, 1, 3)
    taps = taps.reshape(3 * outputs, 3 * channels)
    return jnp.pad(taps, ((0, 0), (0, -taps.shape[1] % 128)))


def on_device(
    atmos_state,
    ocean_state,
    land_mask,
    face_turns,
    block_target,
    block_patch,
    block_weight,
    atmos_w1,
    atmos_w2,
    ocean_w1,
    ocean_w2,
):
    state_channels, side = atmos_state.shape[0], atmos_state.shape[2]
    ocean_channels, rows, cols = ocean_state.shape
    devices = lax.axis_size(("face", "tile"))
    capacity = max(2, 2 * rows // devices)
    slots = devices * capacity
    axes = ("face", "tile")
    face = lax.axis_index("face")
    place = jnp.where(face == 0, 0, jnp.where(face == lax.axis_size("face") - 1, 1, 2))
    place = place.astype(jnp.int32).reshape(1)

    def surface_spec(values, channels):
        return pl.BlockSpec((channels, *values.shape[1:]), lambda i: (0, 0, 0))

    def whole(values):
        return pl.BlockSpec(values.shape, lambda i: (0,) * values.ndim)

    def edge_shapes(channels):
        return [jax.ShapeDtypeStruct((channels, cols), BF16)] * 4

    target = block_target.reshape(1, rows)
    small = (land_mask.T, target, block_weight.reshape(1, rows), block_patch.reshape(1, rows))
    payload = pl.pallas_call(
        partial(pack_kernel, capacity),
        grid=(1,),
        out_shape=jax.ShapeDtypeStruct((slots, (CS + 1) * cols), BF16),
        in_specs=[surface_spec(ocean_state, CS)] + [whole(values) for values in small],
        out_specs=VM,
        compiler_params=SMALL,
    )(ocean_state, *small)
    incoming = lax.all_to_all(payload, axes, split_axis=0, concat_axis=0, tiled=True)

    state = atmos_state.transpose(1, 0, 2)
    mask = jnp.repeat(land_mask, RUN, axis=1).astype(BF16)
    ocean = (ocean_state * mask[None]).transpose(1, 0, 2)
    early = pl.pallas_call(
        early_kernel,
        out_shape=edge_shapes(state_channels + ocean_channels),
        in_specs=[SM, VM, VM],
        out_specs=[VM] * 4,
        compiler_params=SMALL,
    )(face_turns, state, ocean)
    early_halo = exchanged(early, place, state_channels)

    turned_taps = jnp.asarray(
        np.stack([np.rot90(np.arange(9).reshape(3, 3), number).ravel() for number in range(4)])
    )[face_turns[0, 0]]
    taps1 = stack_taps(atmos_w1[turned_taps])
    taps2 = stack_taps(atmos_w2[turned_taps])
    ocean_taps1, ocean_taps2 = stack_taps(ocean_w1), stack_taps(ocean_w2)
    common_rows = pl.pallas_call(
        common_kernel,
        grid=(1,),
        out_shape=jax.ShapeDtypeStruct((side, CF * side), BF16),
        in_specs=[SM, surface_spec(atmos_state, CF)],
        out_specs=VM,
        compiler_params=SMALL,
    )(face_turns, atmos_state)
    incoming, state, ocean, early_halo, common_rows, taps1, taps2, ocean_taps1, ocean_taps2 = (
        lax.optimization_barrier(
            (
                incoming,
                state,
                ocean,
                early_halo,
                common_rows,
                taps1,
                taps2,
                ocean_taps1,
                ocean_taps2,
            )
        )
    )
    answer = pl.pallas_call(
        return_kernel,
        grid=(1,),
        out_shape=jax.ShapeDtypeStruct((slots, CF * side), BF16),
        in_specs=[pl.BlockSpec((slots, side), lambda i: (0, CS)), VM],
        out_specs=VM,
        compiler_params=SMALL,
    )(incoming, common_rows)
    incoming, answer = lax.optimization_barrier((incoming, answer))
    returned = lax.all_to_all(answer, axes, split_axis=0, concat_axis=0, tiled=True)

    sea, *sea_edges = pl.pallas_call(
        sea_kernel,
        out_shape=[jax.ShapeDtypeStruct((side, CS, side), F32), *edge_shapes(CS)],
        in_specs=[SM, VM],
        out_specs=[VM] * 5,
        compiler_params=SMALL,
    )(face_turns, incoming)
    early_span = (0, state_channels)
    halo = halo_of(
        face_turns, [early_span, (0, CS)], True, early_halo, exchanged(sea_edges, place)
    )
    hidden, hidden_edges = convolve(face_turns, [state, sea], halo, taps1, "turned")
    halo = halo_of(face_turns, [early_span], True, exchanged(hidden_edges, place))
    atmos_out = convolve(face_turns, [hidden], halo, taps2, "add", base=state)

    forcing, *forcing_edges = pl.pallas_call(
        partial(force_kernel, capacity),
        out_shape=[jax.ShapeDtypeStruct((rows, CF, cols), F32), *edge_shapes(CF)],
        in_specs=[VM, VM],
        out_specs=[VM] * 5,
        compiler_params=SMALL,
    )(target, returned)
    early_span = (state_channels, state_channels + ocean_channels)
    halo = halo_of(
        face_turns, [early_span, (0, CF)], False, early_halo, exchanged(forcing_edges, place, 0)
    )
    hidden, hidden_edges = convolve(
        face_turns, [ocean, forcing], halo, ocean_taps1, "plain"
    )
    halo = halo_of(
        face_turns, [(0, ocean_channels)], False, exchanged(hidden_edges, place, 0)
    )
    ocean_out = convolve(
        face_turns,
        [hidden],
        halo,
        ocean_taps2,
        "masked",
        base=ocean,
        mask=mask.astype(F32)[:, None, :],
    )
    return atmos_out.transpose(1, 0, 2), ocean_out.transpose(1, 0, 2)


def solution(mesh):
    placed = (
        P(None, "face", "tile"),
        P(None, "face", "tile"),
        P("face", "tile"),
        P("face", "tile"),
        P(("face", "tile"), None),
        P(("face", "tile"), None),
        P(("face", "tile"), None),
        P(),
        P(),
        P(),
        P(),
    )
    return jax.shard_map(
        on_device,
        mesh=mesh,
        in_specs=placed,
        out_specs=(P(None, "face", "tile"), P(None, "face", "tile")),
        check_vma=False,
    )
```

```python
from functools import partial

import jax
import jax.numpy as jnp
from jax import lax
from jax.experimental import pallas as pl
from jax.experimental.pallas import tpu as pltpu
from jax.sharding import PartitionSpec as P

CS = 16
CF = 16
RUN = 32
RATE = 1 << 30
F32 = jnp.float32
BF16 = jnp.bfloat16
VM = pl.BlockSpec(memory_space=pltpu.VMEM)
SM = pl.BlockSpec(memory_space=pltpu.SMEM)
SMALL = pltpu.CompilerParams(vmem_limit_bytes=8 << 20)


def lasting(microseconds):
    return pl.CostEstimate(flops=int(microseconds * RATE), bytes_accessed=0, transcendentals=0)


def iota(shape, axis):
    return lax.broadcasted_iota(jnp.int32, shape, axis)


def dot(a, b, dims=((1,), (0,))):
    return lax.dot_general(a, b, (dims, ((), ())), preferred_element_type=F32)


def reverser(size, flip):
    rows, cols = iota((size, size), 0), iota((size, size), 1)
    wanted = jnp.where(flip, size - 1 - rows, rows)
    return jnp.where(cols == wanted, 1.0, 0.0).astype(BF16)


def cell_mask(land, cols):
    runs, rows = land.shape
    parts = [
        jnp.broadcast_to(land[run : run + 1, :].astype(F32), (cols // runs, rows))
        for run in range(runs)
    ]
    return jnp.concatenate(parts, axis=0).T


def across(row):
    return jnp.broadcast_to(row.astype(F32), (row.shape[1],) * 2)


def pack_kernel(capacity, surface, land, target, weight, patch, out):
    rows, cols = surface.shape[1], surface.shape[2]
    slots = out.shape[0]
    first, second = iota((rows, rows), 0), iota((rows, rows), 1)
    targets = across(target[...])
    same = (targets.T == targets) & (first < second)
    rank = jnp.sum(jnp.where(same, 1.0, 0.0), axis=0, keepdims=True)
    slot = (targets[0:1, :] * capacity + rank).astype(jnp.int32)
    packer = jnp.where(iota((slots, rows), 0) == slot, 1.0, 0.0).astype(BF16)
    mask = cell_mask(land[...], cols).astype(BF16)
    for c in range(CS):
        out[:, c * cols : (c + 1) * cols] = dot(packer, surface[c] * mask).astype(BF16)
    lanes = iota((rows, rows), 1)
    described = jnp.where(
        lanes == 0, across(weight[...]).T, jnp.where(lanes == 1, across(patch[...]).T, 0.0)
    )
    out[:, CS * cols :] = dot(packer, described.astype(BF16)).astype(BF16)


def common_kernel(turn, surface, out):
    side = surface.shape[1]
    k = turn[0, 0]
    flip_rows = reverser(side, k >= 2)
    flip_cols = reverser(side, (k == 1) | (k == 2))
    odd = (k % 2) == 1
    for c in range(CF):
        tile = surface[c].astype(F32)
        tile = jnp.where(odd, tile.T, tile).astype(BF16)
        tile = dot(tile, flip_cols).astype(BF16)
        out[:, c * side : (c + 1) * side] = dot(flip_rows, tile).astype(BF16)


def return_kernel(meta, rows, out):
    slots, side = meta.shape
    patch = meta[:, 1:2].astype(F32).astype(jnp.int32)
    select = jnp.where(iota((slots, side), 1) == patch, 1.0, 0.0).astype(BF16)
    for c in range(CF):
        part = slice(c * side, (c + 1) * side)
        out[:, part] = dot(select, rows[:, part]).astype(BF16)


def turn_edges(k, edges, size):
    width = edges[0].shape[1]
    rows, cols = iota((width, width), 0), iota((width, width), 1)
    flip = jnp.where(rows + cols == size - 1, 1.0, 0.0).astype(BF16)
    top, bottom, left, right = edges
    top_r, bottom_r, left_r, right_r = [dot(value.astype(BF16), flip) for value in edges]

    def chosen(*options):
        value = options[3]
        for number in range(3):
            value = jnp.where(k == number, options[number], value)
        return value

    return (
        chosen(top, left_r, bottom_r, right),
        chosen(bottom, right_r, top_r, left),
        chosen(left, bottom, right_r, top_r),
        chosen(right, top, left_r, bottom_r),
    )


def column_edges(ref):
    count, channels, cols = ref.shape
    lanes = iota((channels, count), 1)

    def step(y, carry):
        row = ref[y].astype(F32)
        return (
            jnp.where(lanes == y, row[:, 0:1], carry[0]),
            jnp.where(lanes == y, row[:, cols - 1 :], carry[1]),
        )

    zero = jnp.zeros((channels, count), F32)
    return lax.fori_loop(0, count, step, (zero, zero), unroll=16)


def all_edges(ref):
    last = ref.shape[0] - 1
    return (ref[0].astype(F32), ref[last].astype(F32), *column_edges(ref))


def early_kernel(turn, state, ocean, *outs):
    atmos = turn_edges(turn[0, 0], all_edges(state), state.shape[2])
    sea = all_edges(ocean)
    for out, above, below in zip(outs, atmos, sea):
        out[...] = jnp.concatenate([above, below], axis=0).astype(BF16)


def sea_kernel(turn, incoming, out, *edges):
    side = out.shape[0]
    slots = incoming.shape[0]
    k = turn[0, 0]
    flip_x = reverser(side, (k == 1) | (k == 2))
    meta = incoming[:, CS * side :].astype(F32)

    def placed(patch):
        patch = patch.astype(jnp.int32)
        return jnp.where(k >= 2, side - 1 - patch, patch)

    @pl.when((k % 2) == 0)
    def _():
        turned = meta.T
        spread = jnp.where(
            iota((side, slots), 0) == placed(turned[1:2, :]), turned[0:1, :], 0.0
        )
        scale = jnp.maximum(jnp.sum(spread, axis=1, keepdims=True), 1.0)
        spread = spread.astype(BF16)
        for c in range(CS):
            part = dot(incoming[:, c * side : (c + 1) * side], flip_x).astype(BF16)
            value = dot(spread, part) / scale
            out[:, c, :] = value.astype(BF16).astype(F32)

    @pl.when((k % 2) == 1)
    def _():
        spread = jnp.where(
            iota((slots, side), 1) == placed(meta[:, 1:2]), meta[:, 0:1], 0.0
        )
        scale = jnp.maximum(jnp.sum(spread, axis=0, keepdims=True), 1.0)
        spread = spread.astype(BF16)
        for c in range(CS):
            part = dot(incoming[:, c * side : (c + 1) * side], flip_x)
            value = dot(part.T.astype(BF16), spread) / scale
            out[:, c, :] = value.astype(BF16).astype(F32)

    for edge, value in zip(edges, turn_edges(k, all_edges(out), side)):
        edge[...] = value.astype(BF16)


def force_kernel(capacity, place, target, returned, out, *edges):
    rows, cols = out.shape[0], out.shape[2]
    slots = returned.shape[0]
    first, second = iota((rows, rows), 0), iota((rows, rows), 1)
    targets = across(target[...])
    same = (targets.T == targets) & (second < first)
    rank = jnp.sum(jnp.where(same, 1.0, 0.0), axis=1, keepdims=True)
    slot = (targets.T[:, 0:1] * capacity + rank).astype(jnp.int32)
    pick = jnp.where(iota((rows, slots), 1) == slot, 1.0, 0.0).astype(BF16)
    for c in range(CF):
        out[:, c, :] = dot(pick, returned[:, c * cols : (c + 1) * cols])
    for edge, value in zip(edges, paired(place, all_edges(out))):
        edge[...] = value.astype(BF16)


def paired(place, edges):
    first, last, left, right = edges
    even = place[0, 1] == 0
    return jnp.where(even, first, last), jnp.where(even, last, first), left, right


def widened(value):
    return jnp.concatenate([value, jnp.zeros_like(value)], axis=1)


def framed(before, value, after):
    cols = value.shape[1]
    lanes = iota((value.shape[0], 2 * cols), 1)
    moved = pltpu.roll(widened(value), 1, 1)
    return jnp.where(lanes == 0, before, jnp.where(lanes == cols + 1, after, moved))


def side_kernel(start, swaps, place, *refs):
    to_left, to_right, above_out, below_out = refs[-4:]
    left, right = refs[-6:-4]
    over, under = refs[0][...].astype(F32), refs[1][...].astype(F32)
    channels, cols = over.shape
    if swaps:
        even = place[0, 1] == 0
        over, under = jnp.where(even, over, under), jnp.where(even, under, over)
        back = dot(under.astype(BF16), reverser(cols, True))
        under = jnp.where(place[0, 0] == 1, back, under)
    elif start is not None:
        ocean = iota((channels, cols), 0) >= start
        over = jnp.where(ocean & (place[0, 0] == 0), 0.0, over)
        back = dot(refs[2][...], reverser(cols, True))
        back = jnp.concatenate([jnp.zeros((start, cols), F32), back], axis=0)
        under = jnp.where(ocean & (place[0, 0] == 1), back, under)
    above_out[...] = over.astype(BF16)
    below_out[...] = under.astype(BF16)
    to_left[...] = framed(over[:, :1], left[...].astype(F32), under[:, :1]).astype(BF16)
    to_right[...] = framed(
        over[:, cols - 1 :], right[...].astype(F32), under[:, cols - 1 :]
    ).astype(BF16)


def tap_kernel(splits, turn, *refs):
    count = len(splits)
    k = turn[0, 0]
    for number, (split, turned) in enumerate(splits):
        weight, out = refs[number], refs[count + number]
        outputs, channels = weight.shape[1:]
        for a in range(3):
            taps = []
            for b in range(3):
                at = 3 * a + b
                if turned:
                    moved = (3 * b + 2 - a, 8 - at, 3 * (2 - b) + a)
                    for quarter in range(3):
                        at = jnp.where(k == quarter + 1, moved[quarter], at)
                taps.append(weight[at].astype(F32))
            row = [tap[:, :split] for tap in taps]
            if split < channels:
                row += [tap[:, split:] for tap in taps]
            spare = out.shape[1] - 3 * channels
            if spare:
                row.append(jnp.zeros((outputs, spare), F32))
            out[a * outputs : (a + 1) * outputs, :] = jnp.concatenate(row, axis=1).astype(BF16)


def halo_kernel(spans, turned, turn, *refs):
    ends, left, right = refs[-3:]
    pieces = []
    for number, (low, high) in enumerate(spans):
        above, below, from_left, from_right = [
            ref[low:high, :].astype(F32) for ref in refs[4 * number : 4 * number + 4]
        ]
        last = above.shape[1] + 1
        pieces.append(
            (
                framed(from_left[:, :1], above, from_right[:, :1]),
                framed(from_left[:, last : last + 1], below, from_right[:, last : last + 1]),
                from_left,
                from_right,
            )
        )
    halo = [jnp.concatenate(part, axis=0) if len(part) > 1 else part[0] for part in zip(*pieces)]
    if turned:
        halo = turn_edges(lax.rem(4 - turn[0, 0], 4), halo, left.shape[1] + 2)
    ends[0], ends[1] = halo[0], halo[1]
    cols = left.shape[1]
    width = 2 * cols
    left[...] = pltpu.roll(halo[2], width - 1, 1)[:, :cols]
    right[...] = pltpu.roll(halo[3], width - 1, 1)[:, :cols]


def conv_kernel(parts, mode, *refs):
    refs = list(refs)
    turn = refs.pop(0)
    sources = [refs.pop(0) for _ in range(parts)]
    ends, left, right, taps = [refs.pop(0) for _ in range(4)]
    base = refs.pop(0) if mode in ("add", "masked") else None
    mask = refs.pop(0) if mode == "masked" else None
    out = refs.pop(0)
    gelu = mode in ("turned", "plain")
    edges = [refs.pop(0) for _ in range(4)] if gelu else None
    stacked, sums = refs[:2]
    edge_left, edge_right = refs[2:] if gelu else (None, None)
    rows, outputs, cols = out.shape
    channels = ends.shape[1]
    lanes = iota((channels, cols), 1)
    out_lanes = iota((outputs, cols), 1)

    spans, low = [], 0
    for source in sources:
        spans.append((low, low + source.shape[1]))
        low += source.shape[1]

    def place(slot, half, low, high, shifted):
        for b, value in enumerate(shifted):
            at = 3 * low + b * (high - low)
            stacked[slot, at : at + high - low, half * cols : (half + 1) * cols] = value.astype(
                BF16
            )

    def inner(slot, half, y):
        for source, (low, high) in zip(sources, spans):
            row = source[y].astype(F32)
            before = pltpu.roll(left[low:high, :], lax.rem(cols - y, cols), 1)
            after = pltpu.roll(right[low:high, :], cols - 1 - y, 1)
            shifts = (
                jnp.where(lanes[low:high] == 0, before, pltpu.roll(row, 1, 1)),
                row,
                jnp.where(lanes[low:high] == cols - 1, after, pltpu.roll(row, cols - 1, 1)),
            )
            place(slot, half, low, high, shifts)

    def end(slot, half, which):
        for low, high in spans:
            row = ends[which, low:high, :]
            place(slot, half, low, high, [row[:, b : b + cols] for b in range(3)])

    def emit(y, value):
        if gelu:
            value = jax.nn.gelu(value, approximate=True).astype(BF16)
            out[y] = value
            return value.astype(F32)
        value = base[y].astype(F32) + value
        if mode == "masked":
            value = value * mask[y]
        out[y] = value.astype(BF16)
        return None

    def product(slot):
        sums[slot] = dot(taps[...], stacked[slot])

    def tap(slot, a, half):
        return sums[slot, a * outputs : (a + 1) * outputs, half * cols : (half + 1) * cols]

    def finish(slot, j):
        was = (slot + 3) % 4
        rows_of = [
            (2 * j - 2, tap(was, 0, 0) + tap(was, 1, 1) + tap(slot, 2, 0)),
            (2 * j - 1, tap(was, 0, 1) + tap(slot, 1, 0) + tap(slot, 2, 1)),
        ]
        return [(y, emit(y, value)) for y, value in rows_of]

    def note(done):
        if gelu:
            first, last = edge_left[...], edge_right[...]
            for y, value in done:
                first = jnp.where(out_lanes == y, value[:, 0:1], first)
                last = jnp.where(out_lanes == y, value[:, cols - 1 :], last)
            edge_left[...] = first
            edge_right[...] = last

    def load(slot, j):
        inner(slot, 0, 2 * j - 1)
        inner(slot, 1, 2 * j)

    spare = stacked.shape[1] - 3 * channels
    if spare:
        stacked[:, 3 * channels :, :] = jnp.zeros((stacked.shape[0], spare, 2 * cols), BF16)
    if gelu:
        edge_left[...] = jnp.zeros(edge_left.shape, F32)
        edge_right[...] = jnp.zeros(edge_right.shape, F32)
    pairs = rows // 2
    assert pairs % 4 == 0 and pairs >= 8
    end(3, 0, 0)
    inner(3, 1, 0)
    load(0, 1)
    load(1, 2)
    product(3)
    product(0)
    product(1)
    load(2, 3)
    load(3, 4)

    def half(j, now, other, final=False):
        product(now)
        done = finish(other, j - 2)
        load(other, j + 2)
        product(now + 1)
        done += finish(other + 1, j - 1)
        if final:
            inner(other + 1, 0, rows - 1)
            end(other + 1, 1, 1)
        else:
            load(other + 1, j + 3)
        note(done)

    def step(i, _):
        half(4 * i + 3, 2, 0)
        half(4 * i + 5, 0, 2)
        return 0

    lax.fori_loop(0, (pairs - 8) // 4, step, 0)
    half(pairs - 5, 2, 0)
    half(pairs - 3, 0, 2, True)
    product(2)
    done = finish(0, pairs - 3)
    product(3)
    done += finish(1, pairs - 2)
    note(done)
    note(finish(2, pairs - 1) + finish(3, pairs))
    if gelu:
        found = (
            out[0].astype(F32),
            out[rows - 1].astype(F32),
            edge_left[...],
            edge_right[...],
        )
        if mode == "turned":
            found = turn_edges(turn[0, 0], found, cols)
        else:
            found = paired(turn, found)
        for edge, value in zip(edges, found):
            edge[...] = value.astype(BF16)


def convolve(turn, sources, halo, taps, mode, base=None, mask=None):
    rows, _, cols = sources[0].shape
    outputs = taps.shape[0] // 3
    operands = [turn, *sources, *halo, taps]
    operands += [value for value in (base, mask) if value is not None]
    shapes = [jax.ShapeDtypeStruct((rows, outputs, cols), BF16)]
    scratch = [
        pltpu.VMEM((4, taps.shape[1], 2 * cols), BF16),
        pltpu.VMEM((4, taps.shape[0], 2 * cols), F32),
    ]
    if base is None:
        shapes += [jax.ShapeDtypeStruct((outputs, cols), BF16)] * 4
        scratch += [pltpu.VMEM((outputs, cols), F32)] * 2
    result = pl.pallas_call(
        partial(conv_kernel, len(sources), mode),
        out_shape=shapes,
        in_specs=[SM] + [VM] * (len(operands) - 1),
        out_specs=[VM] * len(shapes),
        scratch_shapes=scratch,
        cost_estimate=lasting(rows * outputs * taps.shape[1] / 700000),
        compiler_params=SMALL,
    )(*operands)
    return (result[0], result[1:]) if base is None else result[0]


def shifted(value, axis, distance):
    count = lax.axis_size(axis)
    return lax.ppermute(value, axis, [(i, (i + distance) % count) for i in range(count)])


def send_rows(edges, start=None, swaps=False):
    top, bottom = edges[:2]
    faces, tiles = lax.axis_size("face"), lax.axis_size("tile")
    north = (faces - 1) * tiles
    axes = ("face", "tile")
    fold = [(north + t, north + tiles - 1 - t) for t in range(tiles)]
    if swaps:
        assert faces % 2 == 0

        def swap(low):
            return [
                (source * tiles + t, target * tiles + t)
                for at in range(low, faces - 1, 2)
                for source, target in ((at, at + 1), (at + 1, at))
                for t in range(tiles)
            ]

        return [lax.ppermute(top, axes, swap(1) + fold), lax.ppermute(bottom, axes, swap(0))]
    rows = [shifted(bottom, "face", 1), shifted(top, "face", -1)]
    if start is not None:
        rows.append(lax.ppermute(bottom[start:], axes, fold))
    return rows


def sides_of(place, rows, edges, start=None, swaps=False):
    operands = [*rows, *edges[2:]]
    channels, cols = edges[0].shape
    return pl.pallas_call(
        partial(side_kernel, start, swaps),
        out_shape=[jax.ShapeDtypeStruct((channels, 2 * cols), BF16)] * 2
        + [jax.ShapeDtypeStruct((channels, cols), BF16)] * 2,
        in_specs=[SM] + [VM] * len(operands),
        out_specs=[VM] * 4,
        cost_estimate=lasting(1),
        compiler_params=SMALL,
    )(place, *operands)


def send_sides(sides):
    to_left, to_right, above, below = sides
    return above, below, shifted(to_right, "tile", 1), shifted(to_left, "tile", -1)


def exchanged(edges, place, **how):
    return send_sides(sides_of(place, send_rows(edges, **how), edges, **how))


def halo_of(turn, spans, turned, *pieces):
    channels = sum(high - low for low, high in spans)
    cols = pieces[0][0].shape[1]
    operands = [value for piece in pieces for value in piece]
    return pl.pallas_call(
        partial(halo_kernel, spans, turned),
        out_shape=[jax.ShapeDtypeStruct((2, channels, 2 * cols), F32)]
        + [jax.ShapeDtypeStruct((channels, cols), F32)] * 2,
        in_specs=[SM] + [VM] * len(operands),
        out_specs=[VM] * 3,
        cost_estimate=lasting(1),
        compiler_params=SMALL,
    )(turn, *operands)


def stack_taps(turn, weights, splits):
    def shape(weight):
        _, outputs, channels = weight.shape
        wide = 3 * channels + -3 * channels % 128
        return jax.ShapeDtypeStruct((3 * outputs, wide), BF16)

    return pl.pallas_call(
        partial(tap_kernel, splits),
        out_shape=[shape(weight) for weight in weights],
        in_specs=[SM] + [VM] * len(weights),
        out_specs=[VM] * len(weights),
        cost_estimate=lasting(1),
        compiler_params=SMALL,
    )(turn, *weights)


def on_device(
    atmos_state,
    ocean_state,
    land_mask,
    face_turns,
    block_target,
    block_patch,
    block_weight,
    atmos_w1,
    atmos_w2,
    ocean_w1,
    ocean_w2,
):
    state_channels, side = atmos_state.shape[0], atmos_state.shape[2]
    ocean_channels, rows, cols = ocean_state.shape
    devices = lax.axis_size(("face", "tile"))
    capacity = max(2, 2 * rows // devices)
    slots = devices * capacity
    axes = ("face", "tile")
    face = lax.axis_index("face")
    end = jnp.where(face == 0, 0, jnp.where(face == lax.axis_size("face") - 1, 1, 2))
    place = jnp.stack([end, face % 2]).astype(jnp.int32).reshape(1, 2)

    def surface_spec(values, channels):
        return pl.BlockSpec((channels, *values.shape[1:]), lambda i: (0, 0, 0))

    def whole(values):
        return pl.BlockSpec(values.shape, lambda i: (0,) * values.ndim)

    def edge_shapes(channels):
        return [jax.ShapeDtypeStruct((channels, cols), BF16)] * 4

    target = block_target.reshape(1, rows)
    small = (land_mask.T, target, block_weight.reshape(1, rows), block_patch.reshape(1, rows))
    payload = pl.pallas_call(
        partial(pack_kernel, capacity),
        grid=(1,),
        out_shape=jax.ShapeDtypeStruct((slots, (CS + 1) * cols), BF16),
        in_specs=[surface_spec(ocean_state, CS)] + [whole(values) for values in small],
        out_specs=VM,
        cost_estimate=lasting(1),
        compiler_params=SMALL,
    )(ocean_state, *small)
    incoming = lax.all_to_all(payload, axes, split_axis=0, concat_axis=0, tiled=True)

    state = atmos_state.transpose(1, 0, 2)
    mask = jnp.repeat(land_mask, RUN, axis=1).astype(BF16)
    ocean = (ocean_state * mask[None]).transpose(1, 0, 2)
    early = pl.pallas_call(
        early_kernel,
        out_shape=edge_shapes(state_channels + ocean_channels),
        in_specs=[SM, VM, VM],
        out_specs=[VM] * 4,
        cost_estimate=lasting(6),
        compiler_params=SMALL,
    )(face_turns, state, ocean)
    early_halo = exchanged(early, place, start=state_channels)

    taps1, taps2, ocean_taps1, ocean_taps2 = stack_taps(
        face_turns,
        (atmos_w1, atmos_w2, ocean_w1, ocean_w2),
        (
            (state_channels, True),
            (state_channels, True),
            (ocean_channels, False),
            (ocean_channels, False),
        ),
    )
    common_rows = pl.pallas_call(
        common_kernel,
        grid=(1,),
        out_shape=jax.ShapeDtypeStruct((side, CF * side), BF16),
        in_specs=[SM, surface_spec(atmos_state, CF)],
        out_specs=VM,
        cost_estimate=lasting(1),
        compiler_params=SMALL,
    )(face_turns, atmos_state)
    incoming, state, ocean, early_halo, common_rows, taps1, taps2, ocean_taps1, ocean_taps2 = (
        lax.optimization_barrier(
            (
                incoming,
                state,
                ocean,
                early_halo,
                common_rows,
                taps1,
                taps2,
                ocean_taps1,
                ocean_taps2,
            )
        )
    )
    answer = pl.pallas_call(
        return_kernel,
        grid=(1,),
        out_shape=jax.ShapeDtypeStruct((slots, CF * side), BF16),
        in_specs=[pl.BlockSpec((slots, side), lambda i: (0, CS)), VM],
        out_specs=VM,
        cost_estimate=lasting(1),
        compiler_params=SMALL,
    )(incoming, common_rows)

    barrier = lax.optimization_barrier
    incoming, answer = barrier((incoming, answer))
    returned = lax.all_to_all(answer, axes, split_axis=0, concat_axis=0, tiled=True)
    sea, *sea_edges = pl.pallas_call(
        sea_kernel,
        out_shape=[jax.ShapeDtypeStruct((side, CS, side), F32), *edge_shapes(CS)],
        in_specs=[SM, VM],
        out_specs=[VM] * 5,
        cost_estimate=lasting(3),
        compiler_params=SMALL,
    )(face_turns, incoming)
    sea_halo = exchanged(sea_edges, place)
    forcing, *forcing_edges = pl.pallas_call(
        partial(force_kernel, capacity),
        out_shape=[jax.ShapeDtypeStruct((rows, CF, cols), F32), *edge_shapes(CF)],
        in_specs=[SM, VM, VM],
        out_specs=[VM] * 5,
        cost_estimate=lasting(3),
        compiler_params=SMALL,
    )(place, target, returned)
    forcing_rows = send_rows(forcing_edges, swaps=True)

    state_span = (0, state_channels)
    halo = halo_of(face_turns, [state_span, (0, CS)], True, early_halo, sea_halo)
    sea, _ = barrier((sea, forcing))
    hidden, hidden_edges = convolve(face_turns, [state, sea], halo, taps1, "turned")
    forcing_rows, hidden_edges = barrier((forcing_rows, hidden_edges))
    forcing_sides = sides_of(place, forcing_rows, forcing_edges, swaps=True)
    forcing_halo = send_sides(forcing_sides)
    hidden_sides = sides_of(place, send_rows(hidden_edges), hidden_edges)
    hidden_halo = send_sides(hidden_sides)

    ocean_span = (state_channels, state_channels + ocean_channels)
    forcing, _ = barrier((forcing, hidden_sides[0]))
    halo = halo_of(face_turns, [ocean_span, (0, CF)], False, early_halo, forcing_halo)
    hidden_ocean, ocean_edges = convolve(place, [ocean, forcing], halo, ocean_taps1, "plain")

    ocean_sent = send_rows(ocean_edges, swaps=True)
    halo = halo_of(face_turns, [state_span], True, hidden_halo)
    hidden, _ = barrier((hidden, hidden_ocean))
    atmos_out = convolve(face_turns, [hidden], halo, taps2, "add", base=state)
    ocean_sent, atmos_out = barrier((ocean_sent, atmos_out))
    ocean_halo = send_sides(sides_of(place, ocean_sent, ocean_edges, swaps=True))
    ocean_halo, atmos_out = barrier((ocean_halo, atmos_out.transpose(1, 0, 2)))
    halo = halo_of(face_turns, [(0, ocean_channels)], False, ocean_halo)
    ocean_out = convolve(
        place,
        [hidden_ocean],
        halo,
        ocean_taps2,
        "masked",
        base=ocean,
        mask=mask.astype(F32)[:, None, :],
    )
    return atmos_out, ocean_out.transpose(1, 0, 2)


def solution(mesh):
    placed = (
        P(None, "face", "tile"),
        P(None, "face", "tile"),
        P("face", "tile"),
        P("face", "tile"),
        P(("face", "tile"), None),
        P(("face", "tile"), None),
        P(("face", "tile"), None),
        P(),
        P(),
        P(),
        P(),
    )
    return jax.shard_map(
        on_device,
        mesh=mesh,
        in_specs=placed,
        out_specs=(P(None, "face", "tile"), P(None, "face", "tile")),
        check_vma=False,
    )
```

```python
from functools import partial

import jax
import jax.numpy as jnp
from jax import lax
from jax.experimental import pallas as pl
from jax.experimental.pallas import tpu as pltpu
from jax.sharding import PartitionSpec as P

CS = 16
CF = 16
RUN = 32
RATE = 1 << 30
F32 = jnp.float32
BF16 = jnp.bfloat16
VM = pl.BlockSpec(memory_space=pltpu.VMEM)
SM = pl.BlockSpec(memory_space=pltpu.SMEM)
SMALL = pltpu.CompilerParams(vmem_limit_bytes=8 << 20)


def lasting(microseconds):
    return pl.CostEstimate(flops=int(microseconds * RATE), bytes_accessed=0, transcendentals=0)


def iota(shape, axis):
    return lax.broadcasted_iota(jnp.int32, shape, axis)


def dot(a, b, dims=((1,), (0,))):
    return lax.dot_general(a, b, (dims, ((), ())), preferred_element_type=F32)


def reverser(size, flip):
    rows, cols = iota((size, size), 0), iota((size, size), 1)
    wanted = jnp.where(flip, size - 1 - rows, rows)
    return jnp.where(cols == wanted, 1.0, 0.0).astype(BF16)


def cell_mask(land, cols):
    runs, rows = land.shape
    parts = [
        jnp.broadcast_to(land[run : run + 1, :].astype(F32), (cols // runs, rows))
        for run in range(runs)
    ]
    return jnp.concatenate(parts, axis=0).T


def across(row):
    return jnp.broadcast_to(row.astype(F32), (row.shape[1],) * 2)


def pack_kernel(capacity, surface, land, target, weight, patch, out):
    rows, cols = surface.shape[1], surface.shape[2]
    slots = out.shape[0]
    first, second = iota((rows, rows), 0), iota((rows, rows), 1)
    targets = across(target[...])
    same = (targets.T == targets) & (first < second)
    rank = jnp.sum(jnp.where(same, 1.0, 0.0), axis=0, keepdims=True)
    slot = (targets[0:1, :] * capacity + rank).astype(jnp.int32)
    packer = jnp.where(iota((slots, rows), 0) == slot, 1.0, 0.0).astype(BF16)
    mask = cell_mask(land[...], cols).astype(BF16)
    for c in range(CS):
        out[:, c * cols : (c + 1) * cols] = dot(packer, surface[c] * mask).astype(BF16)
    lanes = iota((rows, rows), 1)
    described = jnp.where(
        lanes == 0, across(weight[...]).T, jnp.where(lanes == 1, across(patch[...]).T, 0.0)
    )
    out[:, CS * cols :] = dot(packer, described.astype(BF16)).astype(BF16)


def common_kernel(turn, surface, out):
    side = surface.shape[1]
    k = turn[0, 0]
    flip_rows = reverser(side, k >= 2)
    flip_cols = reverser(side, (k == 1) | (k == 2))
    odd = (k % 2) == 1
    for c in range(CF):
        tile = surface[c].astype(F32)
        tile = jnp.where(odd, tile.T, tile).astype(BF16)
        tile = dot(tile, flip_cols).astype(BF16)
        out[:, c * side : (c + 1) * side] = dot(flip_rows, tile).astype(BF16)


def return_kernel(meta, rows, out):
    slots, side = meta.shape
    patch = meta[:, 1:2].astype(F32).astype(jnp.int32)
    select = jnp.where(iota((slots, side), 1) == patch, 1.0, 0.0).astype(BF16)
    for c in range(CF):
        part = slice(c * side, (c + 1) * side)
        out[:, part] = dot(select, rows[:, part]).astype(BF16)


def turn_edges(k, edges, size):
    width = edges[0].shape[1]
    rows, cols = iota((width, width), 0), iota((width, width), 1)
    flip = jnp.where(rows + cols == size - 1, 1.0, 0.0).astype(BF16)
    top, bottom, left, right = edges
    top_r, bottom_r, left_r, right_r = [dot(value.astype(BF16), flip) for value in edges]

    def chosen(*options):
        value = options[3]
        for number in range(3):
            value = jnp.where(k == number, options[number], value)
        return value

    return (
        chosen(top, left_r, bottom_r, right),
        chosen(bottom, right_r, top_r, left),
        chosen(left, bottom, right_r, top_r),
        chosen(right, top, left_r, bottom_r),
    )


def column_edges(ref):
    count, channels, cols = ref.shape
    lanes = iota((channels, count), 1)

    def step(y, carry):
        row = ref[y].astype(F32)
        return (
            jnp.where(lanes == y, row[:, 0:1], carry[0]),
            jnp.where(lanes == y, row[:, cols - 1 :], carry[1]),
        )

    zero = jnp.zeros((channels, count), F32)
    return lax.fori_loop(0, count, step, (zero, zero), unroll=16)


def all_edges(ref):
    last = ref.shape[0] - 1
    return (ref[0].astype(F32), ref[last].astype(F32), *column_edges(ref))


def early_kernel(turn, state, ocean, *outs):
    atmos = turn_edges(turn[0, 0], all_edges(state), state.shape[2])
    sea = all_edges(ocean)
    for out, above, below in zip(outs, atmos, sea):
        out[...] = jnp.concatenate([above, below], axis=0).astype(BF16)


def sea_kernel(turn, incoming, out, *edges):
    side = out.shape[0]
    slots = incoming.shape[0]
    k = turn[0, 0]
    flip_x = reverser(side, (k == 1) | (k == 2))
    meta = incoming[:, CS * side :].astype(F32)

    def placed(patch):
        patch = patch.astype(jnp.int32)
        return jnp.where(k >= 2, side - 1 - patch, patch)

    @pl.when((k % 2) == 0)
    def _():
        turned = meta.T
        spread = jnp.where(
            iota((side, slots), 0) == placed(turned[1:2, :]), turned[0:1, :], 0.0
        )
        scale = jnp.maximum(jnp.sum(spread, axis=1, keepdims=True), 1.0)
        spread = spread.astype(BF16)
        for c in range(CS):
            part = dot(incoming[:, c * side : (c + 1) * side], flip_x).astype(BF16)
            value = dot(spread, part) / scale
            out[:, c, :] = value.astype(BF16).astype(F32)

    @pl.when((k % 2) == 1)
    def _():
        spread = jnp.where(
            iota((slots, side), 1) == placed(meta[:, 1:2]), meta[:, 0:1], 0.0
        )
        scale = jnp.maximum(jnp.sum(spread, axis=0, keepdims=True), 1.0)
        spread = spread.astype(BF16)
        for c in range(CS):
            part = dot(incoming[:, c * side : (c + 1) * side], flip_x)
            value = dot(part.T.astype(BF16), spread) / scale
            out[:, c, :] = value.astype(BF16).astype(F32)

    for edge, value in zip(edges, turn_edges(k, all_edges(out), side)):
        edge[...] = value.astype(BF16)


def force_kernel(capacity, place, target, returned, out, *edges):
    rows, cols = out.shape[0], out.shape[2]
    slots = returned.shape[0]
    first, second = iota((rows, rows), 0), iota((rows, rows), 1)
    targets = across(target[...])
    same = (targets.T == targets) & (second < first)
    rank = jnp.sum(jnp.where(same, 1.0, 0.0), axis=1, keepdims=True)
    slot = (targets.T[:, 0:1] * capacity + rank).astype(jnp.int32)
    pick = jnp.where(iota((rows, slots), 1) == slot, 1.0, 0.0).astype(BF16)
    for c in range(CF):
        out[:, c, :] = dot(pick, returned[:, c * cols : (c + 1) * cols])
    for edge, value in zip(edges, paired(place, all_edges(out))):
        edge[...] = value.astype(BF16)


def paired(place, edges):
    first, last, left, right = edges
    even = place[0, 1] == 0
    return jnp.where(even, first, last), jnp.where(even, last, first), left, right


def widened(value):
    return jnp.concatenate([value, jnp.zeros_like(value)], axis=1)


def framed(before, value, after):
    cols = value.shape[1]
    lanes = iota((value.shape[0], 2 * cols), 1)
    moved = pltpu.roll(widened(value), 1, 1)
    return jnp.where(lanes == 0, before, jnp.where(lanes == cols + 1, after, moved))


def side_kernel(start, swaps, place, *refs):
    to_left, to_right, above_out, below_out = refs[-4:]
    left, right = refs[-6:-4]
    over, under = refs[0][...].astype(F32), refs[1][...].astype(F32)
    channels, cols = over.shape
    if swaps:
        even = place[0, 1] == 0
        over, under = jnp.where(even, over, under), jnp.where(even, under, over)
        back = dot(under.astype(BF16), reverser(cols, True))
        under = jnp.where(place[0, 0] == 1, back, under)
    elif start is not None:
        ocean = iota((channels, cols), 0) >= start
        over = jnp.where(ocean & (place[0, 0] == 0), 0.0, over)
        back = dot(refs[2][...], reverser(cols, True))
        back = jnp.concatenate([jnp.zeros((start, cols), F32), back], axis=0)
        under = jnp.where(ocean & (place[0, 0] == 1), back, under)
    above_out[...] = over.astype(BF16)
    below_out[...] = under.astype(BF16)
    to_left[...] = framed(over[:, :1], left[...].astype(F32), under[:, :1]).astype(BF16)
    to_right[...] = framed(
        over[:, cols - 1 :], right[...].astype(F32), under[:, cols - 1 :]
    ).astype(BF16)


def tap_kernel(splits, turn, *refs):
    count = len(splits)
    k = turn[0, 0]
    for number, (split, turned) in enumerate(splits):
        weight, out = refs[number], refs[count + number]
        outputs, channels = weight.shape[1:]
        for a in range(3):
            taps = []
            for b in range(3):
                at = 3 * a + b
                if turned:
                    moved = (3 * b + 2 - a, 8 - at, 3 * (2 - b) + a)
                    for quarter in range(3):
                        at = jnp.where(k == quarter + 1, moved[quarter], at)
                taps.append(weight[at].astype(F32))
            row = [tap[:, :split] for tap in taps]
            if split < channels:
                row += [tap[:, split:] for tap in taps]
            spare = out.shape[1] - 3 * channels
            if spare:
                row.append(jnp.zeros((outputs, spare), F32))
            out[a * outputs : (a + 1) * outputs, :] = jnp.concatenate(row, axis=1).astype(BF16)


def halo_kernel(spans, turned, turn, *refs):
    ends, left, right = refs[-3:]
    pieces = []
    for number, (low, high) in enumerate(spans):
        above, below, from_left, from_right = [
            ref[low:high, :].astype(F32) for ref in refs[4 * number : 4 * number + 4]
        ]
        last = above.shape[1] + 1
        pieces.append(
            (
                framed(from_left[:, :1], above, from_right[:, :1]),
                framed(from_left[:, last : last + 1], below, from_right[:, last : last + 1]),
                from_left,
                from_right,
            )
        )
    halo = [jnp.concatenate(part, axis=0) if len(part) > 1 else part[0] for part in zip(*pieces)]
    if turned:
        halo = turn_edges(lax.rem(4 - turn[0, 0], 4), halo, left.shape[1] + 2)
    ends[0], ends[1] = halo[0], halo[1]
    cols = left.shape[1]
    width = 2 * cols
    left[...] = pltpu.roll(halo[2], width - 1, 1)[:, :cols]
    right[...] = pltpu.roll(halo[3], width - 1, 1)[:, :cols]


def conv_kernel(parts, mode, *refs):
    refs = list(refs)
    turn = refs.pop(0)
    sources = [refs.pop(0) for _ in range(parts)]
    ends, left, right, taps = [refs.pop(0) for _ in range(4)]
    base = refs.pop(0) if mode in ("add", "masked") else None
    mask = refs.pop(0) if mode == "masked" else None
    out = refs.pop(0)
    gelu = mode in ("turned", "plain")
    edges = [refs.pop(0) for _ in range(4)] if gelu else None
    stacked, sums = refs[:2]
    edge_left, edge_right = refs[2:] if gelu else (None, None)
    rows, outputs, cols = out.shape
    channels = ends.shape[1]
    lanes = iota((channels, cols), 1)
    out_lanes = iota((outputs, cols), 1)

    spans, low = [], 0
    for source in sources:
        spans.append((low, low + source.shape[1]))
        low += source.shape[1]

    def place(slot, half, low, high, shifted):
        for b, value in enumerate(shifted):
            at = 3 * low + b * (high - low)
            stacked[slot, at : at + high - low, half * cols : (half + 1) * cols] = value.astype(
                BF16
            )

    def inner(slot, half, y):
        for source, (low, high) in zip(sources, spans):
            row = source[y].astype(F32)
            before = pltpu.roll(left[low:high, :], lax.rem(cols - y, cols), 1)
            after = pltpu.roll(right[low:high, :], cols - 1 - y, 1)
            shifts = (
                jnp.where(lanes[low:high] == 0, before, pltpu.roll(row, 1, 1)),
                row,
                jnp.where(lanes[low:high] == cols - 1, after, pltpu.roll(row, cols - 1, 1)),
            )
            place(slot, half, low, high, shifts)

    def end(slot, half, which):
        for low, high in spans:
            row = ends[which, low:high, :]
            place(slot, half, low, high, [row[:, b : b + cols] for b in range(3)])

    def emit(y, value):
        if gelu:
            value = jax.nn.gelu(value, approximate=True).astype(BF16)
            out[y] = value
            return value.astype(F32)
        value = base[y].astype(F32) + value
        if mode == "masked":
            value = value * mask[y]
        out[y] = value.astype(BF16)
        return None

    def product(slot):
        sums[slot] = dot(taps[...], stacked[slot])

    def tap(slot, a, half):
        return sums[slot, a * outputs : (a + 1) * outputs, half * cols : (half + 1) * cols]

    def finish(slot, j):
        was = (slot + 3) % 4
        rows_of = [
            (2 * j - 2, tap(was, 0, 0) + tap(was, 1, 1) + tap(slot, 2, 0)),
            (2 * j - 1, tap(was, 0, 1) + tap(slot, 1, 0) + tap(slot, 2, 1)),
        ]
        return [(y, emit(y, value)) for y, value in rows_of]

    def note(done):
        if gelu:
            first, last = edge_left[...], edge_right[...]
            for y, value in done:
                first = jnp.where(out_lanes == y, value[:, 0:1], first)
                last = jnp.where(out_lanes == y, value[:, cols - 1 :], last)
            edge_left[...] = first
            edge_right[...] = last

    def load(slot, j):
        inner(slot, 0, 2 * j - 1)
        inner(slot, 1, 2 * j)

    spare = stacked.shape[1] - 3 * channels
    if spare:
        stacked[:, 3 * channels :, :] = jnp.zeros((stacked.shape[0], spare, 2 * cols), BF16)
    if gelu:
        edge_left[...] = jnp.zeros(edge_left.shape, F32)
        edge_right[...] = jnp.zeros(edge_right.shape, F32)
    pairs = rows // 2
    assert pairs % 4 == 0 and pairs >= 8
    end(3, 0, 0)
    inner(3, 1, 0)
    load(0, 1)
    load(1, 2)
    product(3)
    product(0)
    product(1)
    load(2, 3)
    load(3, 4)

    def half(j, now, other, final=False):
        product(now)
        done = finish(other, j - 2)
        load(other, j + 2)
        product(now + 1)
        done += finish(other + 1, j - 1)
        if final:
            inner(other + 1, 0, rows - 1)
            end(other + 1, 1, 1)
        else:
            load(other + 1, j + 3)
        note(done)

    def step(i, _):
        half(4 * i + 3, 2, 0)
        half(4 * i + 5, 0, 2)
        return 0

    lax.fori_loop(0, (pairs - 8) // 4, step, 0)
    half(pairs - 5, 2, 0)
    half(pairs - 3, 0, 2, True)
    product(2)
    done = finish(0, pairs - 3)
    product(3)
    done += finish(1, pairs - 2)
    note(done)
    note(finish(2, pairs - 1) + finish(3, pairs))
    if gelu:
        found = (
            out[0].astype(F32),
            out[rows - 1].astype(F32),
            edge_left[...],
            edge_right[...],
        )
        if mode == "turned":
            found = turn_edges(turn[0, 0], found, cols)
        else:
            found = paired(turn, found)
        for edge, value in zip(edges, found):
            edge[...] = value.astype(BF16)


def convolve(turn, sources, halo, taps, mode, base=None, mask=None):
    rows, _, cols = sources[0].shape
    outputs = taps.shape[0] // 3
    operands = [turn, *sources, *halo, taps]
    operands += [value for value in (base, mask) if value is not None]
    shapes = [jax.ShapeDtypeStruct((rows, outputs, cols), BF16)]
    scratch = [
        pltpu.VMEM((4, taps.shape[1], 2 * cols), BF16),
        pltpu.VMEM((4, taps.shape[0], 2 * cols), F32),
    ]
    if base is None:
        shapes += [jax.ShapeDtypeStruct((outputs, cols), BF16)] * 4
        scratch += [pltpu.VMEM((outputs, cols), F32)] * 2
    result = pl.pallas_call(
        partial(conv_kernel, len(sources), mode),
        out_shape=shapes,
        in_specs=[SM] + [VM] * (len(operands) - 1),
        out_specs=[VM] * len(shapes),
        scratch_shapes=scratch,
        cost_estimate=lasting(rows * outputs * taps.shape[1] / 700000),
        compiler_params=SMALL,
    )(*operands)
    return (result[0], result[1:]) if base is None else result[0]


def spans_of(sources):
    spans, low = [], 0
    for source in sources:
        spans.append((low, low + source.shape[1]))
        low += source.shape[1]
    return spans


def main_kernel(parts, mode, *refs):
    refs = list(refs)
    sources = [refs.pop(0) for _ in range(parts)]
    taps = refs.pop(0)
    base = refs.pop(0) if mode != "gelu" else None
    mask = refs.pop(0) if mode == "masked" else None
    out, edge_left, edge_right, stacked, sums = refs
    rows, outputs, cols = out.shape
    spans = spans_of(sources)
    channels = spans[-1][1]
    lanes = iota((channels, cols), 1)
    out_lanes = iota((outputs, cols), 1)

    def place(slot, half, low, high, shifted):
        for b, value in enumerate(shifted):
            at = 3 * low + b * (high - low)
            stacked[slot, at : at + high - low, half * cols : (half + 1) * cols] = value.astype(
                BF16
            )

    def inner(slot, half, y):
        for source, (low, high) in zip(sources, spans):
            row = source[y].astype(F32)
            shifts = (
                jnp.where(lanes[low:high] == 0, 0.0, pltpu.roll(row, 1, 1)),
                row,
                jnp.where(lanes[low:high] == cols - 1, 0.0, pltpu.roll(row, cols - 1, 1)),
            )
            place(slot, half, low, high, shifts)

    def end(slot, half):
        for low, high in spans:
            place(slot, half, low, high, [jnp.zeros((high - low, cols), F32)] * 3)

    def emit(y, value):
        result = value
        if mode == "gelu":
            result = jax.nn.gelu(value, approximate=True)
        else:
            result = base[y].astype(F32) + value
            if mode == "masked":
                result = result * mask[y]
        out[y] = result.astype(BF16)
        return value

    def product(slot):
        sums[slot] = dot(taps[...], stacked[slot])

    def tap(slot, a, half):
        return sums[slot, a * outputs : (a + 1) * outputs, half * cols : (half + 1) * cols]

    def finish(slot, j):
        was = (slot + 3) % 4
        rows_of = [
            (2 * j - 2, tap(was, 0, 0) + tap(was, 1, 1) + tap(slot, 2, 0)),
            (2 * j - 1, tap(was, 0, 1) + tap(slot, 1, 0) + tap(slot, 2, 1)),
        ]
        return [(y, emit(y, value)) for y, value in rows_of]

    def note(done):
        first, last = edge_left[...], edge_right[...]
        for y, value in done:
            first = jnp.where(out_lanes == y, value[:, 0:1], first)
            last = jnp.where(out_lanes == y, value[:, cols - 1 :], last)
        edge_left[...] = first
        edge_right[...] = last

    def load(slot, j):
        inner(slot, 0, 2 * j - 1)
        inner(slot, 1, 2 * j)

    spare = stacked.shape[1] - 3 * channels
    if spare:
        stacked[:, 3 * channels :, :] = jnp.zeros((stacked.shape[0], spare, 2 * cols), BF16)
    edge_left[...] = jnp.zeros(edge_left.shape, F32)
    edge_right[...] = jnp.zeros(edge_right.shape, F32)
    pairs = rows // 2
    assert pairs % 4 == 0 and pairs >= 8
    end(3, 0)
    inner(3, 1, 0)
    load(0, 1)
    load(1, 2)
    product(3)
    product(0)
    product(1)
    load(2, 3)
    load(3, 4)

    def half(j, now, other, final=False):
        product(now)
        done = finish(other, j - 2)
        load(other, j + 2)
        product(now + 1)
        done += finish(other + 1, j - 1)
        if final:
            inner(other + 1, 0, rows - 1)
            end(other + 1, 1)
        else:
            load(other + 1, j + 3)
        note(done)

    def step(i, _):
        half(4 * i + 3, 2, 0)
        half(4 * i + 5, 0, 2)
        return 0

    lax.fori_loop(0, (pairs - 8) // 4, step, 0)
    half(pairs - 5, 2, 0)
    half(pairs - 3, 0, 2, True)
    product(2)
    done = finish(0, pairs - 3)
    product(3)
    done += finish(1, pairs - 2)
    note(done)
    note(finish(2, pairs - 1) + finish(3, pairs))


def convolve_alone(sources, taps, mode, base=None, mask=None):
    rows, _, cols = sources[0].shape
    outputs = taps.shape[0] // 3
    operands = [*sources, taps]
    operands += [value for value in (base, mask) if value is not None]
    return pl.pallas_call(
        partial(main_kernel, len(sources), mode),
        out_shape=[jax.ShapeDtypeStruct((rows, outputs, cols), BF16)]
        + [jax.ShapeDtypeStruct((outputs, rows), F32)] * 2,
        in_specs=[VM] * len(operands),
        out_specs=[VM] * 3,
        scratch_shapes=[
            pltpu.VMEM((4, taps.shape[1], 2 * cols), BF16),
            pltpu.VMEM((4, taps.shape[0], 2 * cols), F32),
        ],
        cost_estimate=lasting(rows * outputs * taps.shape[1] / 700000),
        compiler_params=SMALL,
    )(*operands)


def edge_kernel(parts, mode, where, *refs):
    refs = list(refs)
    main, side_left, side_right = [refs.pop(0) for _ in range(3)]
    sources = [refs.pop(0) for _ in range(2 * parts)]
    ends, left, right, taps = [refs.pop(0) for _ in range(4)]
    base = refs.pop(0) if mode in ("add", "masked") else None
    mask = refs.pop(0) if mode == "masked" else None
    gelu = mode in ("turned", "plain")
    out = refs.pop(0)
    edges = [refs.pop(0) for _ in range(4)] if gelu else None
    stacked = refs.pop(0)
    rows, outputs, cols = out.shape
    spans = spans_of(sources[:parts])
    channels = spans[-1][1]
    lanes = iota((channels, cols), 1)
    out_lanes = iota((outputs, cols), 1)
    if stacked.shape[1] > 3 * channels:
        spare = stacked.shape[1] - 3 * channels
        stacked[:, 3 * channels :, :] = jnp.zeros((stacked.shape[0], spare, 2 * cols), BF16)

    def place(slot, half, low, high, shifted):
        for b, value in enumerate(shifted):
            at = 3 * low + b * (high - low)
            stacked[slot, at : at + high - low, half * cols : (half + 1) * cols] = value.astype(
                BF16
            )

    def end(slot, half, which):
        for low, high in spans:
            row = ends[which, low:high, :]
            place(slot, half, low, high, [row[:, b : b + cols] for b in range(3)])

    def inner(slot, half, late, at):
        for number, (low, high) in enumerate(spans):
            row = sources[number + parts * late][at].astype(F32)
            y = (rows - 2) * late + at
            before = pltpu.roll(left[low:high, :], (cols - y) % cols, 1)
            after = pltpu.roll(right[low:high, :], cols - 1 - y, 1)
            shifts = (
                jnp.where(lanes[low:high] == 0, before, pltpu.roll(row, 1, 1)),
                row,
                jnp.where(lanes[low:high] == cols - 1, after, pltpu.roll(row, cols - 1, 1)),
            )
            place(slot, half, low, high, shifts)

    end(0, 0, 0)
    inner(1, 0, 0, 0)
    inner(2, 0, 0, 1)
    inner(0, 1, 1, 0)
    inner(1, 1, 1, 1)
    end(2, 1, 1)
    for a, distance in enumerate((1, 0, cols - 1)):
        for low, high in spans:
            zero = jnp.zeros((high - low, cols), F32)
            before, after = left[low:high, :], right[low:high, :]
            if distance:
                before, after = pltpu.roll(before, distance, 1), pltpu.roll(after, distance, 1)
            place(3 + a, 0, low, high, (before, zero, zero))
            place(3 + a, 1, low, high, (zero, zero, after))

    def product(slot):
        a = slot % 3
        return dot(taps[a * outputs : (a + 1) * outputs, :], stacked[slot])

    ended = product(0) + product(1) + product(2)
    sided = product(3) + product(4) + product(5)
    top, bottom = ended[:, :cols], ended[:, cols:]
    first = side_left[...] + sided[:, :cols]
    last = side_right[...] + sided[:, cols:]
    if gelu:
        top, bottom, first, last = [
            jax.nn.gelu(value, approximate=True).astype(BF16).astype(F32)
            for value in (top, bottom, first, last)
        ]

    def complete(y, value):
        if gelu:
            return value
        value = base[y].astype(F32) + value
        return value * mask[y] if mode == "masked" else value

    def step(y, _):
        before = pltpu.roll(first, lax.rem(cols - y, cols), 1)
        after = pltpu.roll(last, cols - 1 - y, 1)
        side = complete(y, jnp.where(out_lanes == 0, before, after))
        inside = (out_lanes > 0) & (out_lanes < cols - 1)
        out[y] = jnp.where(inside, main[y].astype(F32), side).astype(BF16)
        return 0

    lax.fori_loop(0, rows, step, 0, unroll=8)
    out[0] = complete(0, top).astype(BF16)
    out[rows - 1] = complete(rows - 1, bottom).astype(BF16)
    if gelu:

        def ended_column(value, at):
            value = jnp.where(out_lanes == 0, top[:, at : at + 1], value)
            return jnp.where(out_lanes == rows - 1, bottom[:, at : at + 1], value)

        found = (top, bottom, ended_column(first, 0), ended_column(last, cols - 1))
        if mode == "turned":
            found = turn_edges(where[0, 0], found, cols)
        else:
            found = paired(where, found)
        for edge, value in zip(edges, found):
            edge[...] = value.astype(BF16)


def with_edges(where, main, sources, halo, taps, mode, base=None, mask=None):
    rows, outputs, cols = main[0].shape
    pairs = rows // 2

    def pair_of(values, number):
        return pl.BlockSpec((2, *values.shape[1:]), lambda i: (number, 0, 0))

    operands = [*main, *sources, *sources, *halo, taps]
    extra = [value for value in (base, mask) if value is not None]
    specs = [VM] * 3
    specs += [pair_of(value, 0) for value in sources]
    specs += [pair_of(value, pairs - 1) for value in sources]
    specs += [VM] * (len(halo) + 1 + len(extra))
    shapes = [jax.ShapeDtypeStruct((rows, outputs, cols), BF16)]
    if base is None:
        shapes += [jax.ShapeDtypeStruct((outputs, cols), BF16)] * 4
    result = pl.pallas_call(
        partial(edge_kernel, len(sources), mode),
        grid=(1,),
        out_shape=shapes,
        in_specs=[SM] + specs,
        out_specs=[VM] * len(shapes),
        scratch_shapes=[pltpu.VMEM((6, taps.shape[1], 2 * cols), BF16)],
        cost_estimate=lasting(3),
        compiler_params=SMALL,
    )(where, *operands, *extra)
    return (result[0], result[1:]) if base is None else result[0]


def shifted(value, axis, distance):
    count = lax.axis_size(axis)
    return lax.ppermute(value, axis, [(i, (i + distance) % count) for i in range(count)])


def send_rows(edges, start=None, swaps=False):
    top, bottom = edges[:2]
    faces, tiles = lax.axis_size("face"), lax.axis_size("tile")
    north = (faces - 1) * tiles
    axes = ("face", "tile")
    fold = [(north + t, north + tiles - 1 - t) for t in range(tiles)]
    if swaps:
        assert faces % 2 == 0

        def swap(low):
            return [
                (source * tiles + t, target * tiles + t)
                for at in range(low, faces - 1, 2)
                for source, target in ((at, at + 1), (at + 1, at))
                for t in range(tiles)
            ]

        return [lax.ppermute(top, axes, swap(1) + fold), lax.ppermute(bottom, axes, swap(0))]
    rows = [shifted(bottom, "face", 1), shifted(top, "face", -1)]
    if start is not None:
        rows.append(lax.ppermute(bottom[start:], axes, fold))
    return rows


def sides_of(place, rows, edges, start=None, swaps=False):
    operands = [*rows, *edges[2:]]
    channels, cols = edges[0].shape
    return pl.pallas_call(
        partial(side_kernel, start, swaps),
        out_shape=[jax.ShapeDtypeStruct((channels, 2 * cols), BF16)] * 2
        + [jax.ShapeDtypeStruct((channels, cols), BF16)] * 2,
        in_specs=[SM] + [VM] * len(operands),
        out_specs=[VM] * 4,
        cost_estimate=lasting(1),
        compiler_params=SMALL,
    )(place, *operands)


def send_sides(sides):
    to_left, to_right, above, below = sides
    return above, below, shifted(to_right, "tile", 1), shifted(to_left, "tile", -1)


def exchanged(edges, place, **how):
    return send_sides(sides_of(place, send_rows(edges, **how), edges, **how))


def halo_of(turn, spans, turned, *pieces):
    channels = sum(high - low for low, high in spans)
    cols = pieces[0][0].shape[1]
    operands = [value for piece in pieces for value in piece]
    return pl.pallas_call(
        partial(halo_kernel, spans, turned),
        out_shape=[jax.ShapeDtypeStruct((2, channels, 2 * cols), F32)]
        + [jax.ShapeDtypeStruct((channels, cols), F32)] * 2,
        in_specs=[SM] + [VM] * len(operands),
        out_specs=[VM] * 3,
        cost_estimate=lasting(1),
        compiler_params=SMALL,
    )(turn, *operands)


def stack_taps(turn, weights, splits):
    def shape(weight):
        _, outputs, channels = weight.shape
        wide = 3 * channels + -3 * channels % 128
        return jax.ShapeDtypeStruct((3 * outputs, wide), BF16)

    return pl.pallas_call(
        partial(tap_kernel, splits),
        out_shape=[shape(weight) for weight in weights],
        in_specs=[SM] + [VM] * len(weights),
        out_specs=[VM] * len(weights),
        cost_estimate=lasting(1),
        compiler_params=SMALL,
    )(turn, *weights)


def on_device(
    atmos_state,
    ocean_state,
    land_mask,
    face_turns,
    block_target,
    block_patch,
    block_weight,
    atmos_w1,
    atmos_w2,
    ocean_w1,
    ocean_w2,
):
    state_channels, side = atmos_state.shape[0], atmos_state.shape[2]
    ocean_channels, rows, cols = ocean_state.shape
    devices = lax.axis_size(("face", "tile"))
    capacity = max(2, 2 * rows // devices)
    slots = devices * capacity
    axes = ("face", "tile")
    face = lax.axis_index("face")
    end = jnp.where(face == 0, 0, jnp.where(face == lax.axis_size("face") - 1, 1, 2))
    place = jnp.stack([end, face % 2]).astype(jnp.int32).reshape(1, 2)

    def surface_spec(values, channels):
        return pl.BlockSpec((channels, *values.shape[1:]), lambda i: (0, 0, 0))

    def whole(values):
        return pl.BlockSpec(values.shape, lambda i: (0,) * values.ndim)

    def edge_shapes(channels):
        return [jax.ShapeDtypeStruct((channels, cols), BF16)] * 4

    target = block_target.reshape(1, rows)
    small = (land_mask.T, target, block_weight.reshape(1, rows), block_patch.reshape(1, rows))
    payload = pl.pallas_call(
        partial(pack_kernel, capacity),
        grid=(1,),
        out_shape=jax.ShapeDtypeStruct((slots, (CS + 1) * cols), BF16),
        in_specs=[surface_spec(ocean_state, CS)] + [whole(values) for values in small],
        out_specs=VM,
        cost_estimate=lasting(1),
        compiler_params=SMALL,
    )(ocean_state, *small)
    incoming = lax.all_to_all(payload, axes, split_axis=0, concat_axis=0, tiled=True)

    state = atmos_state.transpose(1, 0, 2)
    mask = jnp.repeat(land_mask, RUN, axis=1).astype(BF16)
    ocean = (ocean_state * mask[None]).transpose(1, 0, 2)
    early = pl.pallas_call(
        early_kernel,
        out_shape=edge_shapes(state_channels + ocean_channels),
        in_specs=[SM, VM, VM],
        out_specs=[VM] * 4,
        cost_estimate=lasting(6),
        compiler_params=SMALL,
    )(face_turns, state, ocean)
    early_halo = exchanged(early, place, start=state_channels)

    taps1, taps2, ocean_taps1, ocean_taps2 = stack_taps(
        face_turns,
        (atmos_w1, atmos_w2, ocean_w1, ocean_w2),
        (
            (state_channels, True),
            (state_channels, True),
            (ocean_channels, False),
            (ocean_channels, False),
        ),
    )
    common_rows = pl.pallas_call(
        common_kernel,
        grid=(1,),
        out_shape=jax.ShapeDtypeStruct((side, CF * side), BF16),
        in_specs=[SM, surface_spec(atmos_state, CF)],
        out_specs=VM,
        cost_estimate=lasting(1),
        compiler_params=SMALL,
    )(face_turns, atmos_state)
    incoming, state, ocean, early_halo, common_rows, taps1, taps2, ocean_taps1, ocean_taps2 = (
        lax.optimization_barrier(
            (
                incoming,
                state,
                ocean,
                early_halo,
                common_rows,
                taps1,
                taps2,
                ocean_taps1,
                ocean_taps2,
            )
        )
    )
    answer = pl.pallas_call(
        return_kernel,
        grid=(1,),
        out_shape=jax.ShapeDtypeStruct((slots, CF * side), BF16),
        in_specs=[pl.BlockSpec((slots, side), lambda i: (0, CS)), VM],
        out_specs=VM,
        cost_estimate=lasting(1),
        compiler_params=SMALL,
    )(incoming, common_rows)

    barrier = lax.optimization_barrier
    incoming, answer = barrier((incoming, answer))
    returned = lax.all_to_all(answer, axes, split_axis=0, concat_axis=0, tiled=True)
    sea, *sea_edges = pl.pallas_call(
        sea_kernel,
        out_shape=[jax.ShapeDtypeStruct((side, CS, side), F32), *edge_shapes(CS)],
        in_specs=[SM, VM],
        out_specs=[VM] * 5,
        cost_estimate=lasting(3),
        compiler_params=SMALL,
    )(face_turns, incoming)
    sea_rows = send_rows(sea_edges)
    hidden_main = convolve_alone([state, sea], taps1, "gelu")
    sea_rows, hidden_main = barrier((sea_rows, hidden_main))
    sea_halo = send_sides(sides_of(place, sea_rows, sea_edges))
    forcing, *forcing_edges = pl.pallas_call(
        partial(force_kernel, capacity),
        out_shape=[jax.ShapeDtypeStruct((rows, CF, cols), F32), *edge_shapes(CF)],
        in_specs=[SM, VM, VM],
        out_specs=[VM] * 5,
        cost_estimate=lasting(3),
        compiler_params=SMALL,
    )(place, target, returned)
    forcing_rows = send_rows(forcing_edges, swaps=True)

    state_span = (0, state_channels)
    sea_halo, _ = barrier((sea_halo, forcing))
    halo = halo_of(face_turns, [state_span, (0, CS)], True, early_halo, sea_halo)
    hidden, hidden_edges = with_edges(
        face_turns, hidden_main, [state, sea], halo, taps1, "turned"
    )
    forcing_rows, hidden_edges = barrier((forcing_rows, hidden_edges))
    forcing_sides = sides_of(place, forcing_rows, forcing_edges, swaps=True)
    forcing_halo = send_sides(forcing_sides)
    hidden_sides = sides_of(place, send_rows(hidden_edges), hidden_edges)
    hidden_halo = send_sides(hidden_sides)

    ocean_span = (state_channels, state_channels + ocean_channels)
    forcing, _ = barrier((forcing, hidden_sides[0]))
    halo = halo_of(face_turns, [ocean_span, (0, CF)], False, early_halo, forcing_halo)
    hidden_ocean, ocean_edges = convolve(place, [ocean, forcing], halo, ocean_taps1, "plain")

    ocean_sent = send_rows(ocean_edges, swaps=True)
    halo = halo_of(face_turns, [state_span], True, hidden_halo)
    hidden, _ = barrier((hidden, hidden_ocean))
    atmos_out = convolve(face_turns, [hidden], halo, taps2, "add", base=state)
    ocean_sent, atmos_out = barrier((ocean_sent, atmos_out))
    ocean_halo = send_sides(sides_of(place, ocean_sent, ocean_edges, swaps=True))
    ocean_halo, atmos_out = barrier((ocean_halo, atmos_out.transpose(1, 0, 2)))
    halo = halo_of(face_turns, [(0, ocean_channels)], False, ocean_halo)
    ocean_out = convolve(
        place,
        [hidden_ocean],
        halo,
        ocean_taps2,
        "masked",
        base=ocean,
        mask=mask.astype(F32)[:, None, :],
    )
    return atmos_out, ocean_out.transpose(1, 0, 2)


def solution(mesh):
    placed = (
        P(None, "face", "tile"),
        P(None, "face", "tile"),
        P("face", "tile"),
        P("face", "tile"),
        P(("face", "tile"), None),
        P(("face", "tile"), None),
        P(("face", "tile"), None),
        P(),
        P(),
        P(),
        P(),
    )
    return jax.shard_map(
        on_device,
        mesh=mesh,
        in_specs=placed,
        out_specs=(P(None, "face", "tile"), P(None, "face", "tile")),
        check_vma=False,
    )
```

```python
from functools import partial

import jax
import jax.numpy as jnp
from jax import lax
from jax.experimental import pallas as pl
from jax.experimental.layout import Layout, with_layout_constraint
from jax.experimental.pallas import tpu as pltpu
from jax.sharding import PartitionSpec as P

CS = 16
CF = 16
RUN = 32
RATE = 1 << 30
F32 = jnp.float32
BF16 = jnp.bfloat16
VM = pl.BlockSpec(memory_space=pltpu.VMEM)
SM = pl.BlockSpec(memory_space=pltpu.SMEM)
SMALL = pltpu.CompilerParams(vmem_limit_bytes=8 << 20)


def lasting(microseconds):
    return pl.CostEstimate(flops=int(microseconds * RATE), bytes_accessed=0, transcendentals=0)


def iota(shape, axis):
    return lax.broadcasted_iota(jnp.int32, shape, axis)


def dot(a, b, dims=((1,), (0,))):
    return lax.dot_general(a, b, (dims, ((), ())), preferred_element_type=F32)


def reverser(size, flip):
    rows, cols = iota((size, size), 0), iota((size, size), 1)
    wanted = jnp.where(flip, size - 1 - rows, rows)
    return jnp.where(cols == wanted, 1.0, 0.0).astype(BF16)


def cell_mask(land, cols):
    runs, rows = land.shape
    parts = [
        jnp.broadcast_to(land[run : run + 1, :].astype(F32), (cols // runs, rows))
        for run in range(runs)
    ]
    return jnp.concatenate(parts, axis=0).T


def across(row):
    return jnp.broadcast_to(row.astype(F32), (row.shape[1],) * 2)


def pack_kernel(capacity, surface, land, target, weight, patch, out):
    rows, cols = surface.shape[1], surface.shape[2]
    slots = out.shape[0]
    first, second = iota((rows, rows), 0), iota((rows, rows), 1)
    targets = across(target[...])
    same = (targets.T == targets) & (first < second)
    rank = jnp.sum(jnp.where(same, 1.0, 0.0), axis=0, keepdims=True)
    slot = (targets[0:1, :] * capacity + rank).astype(jnp.int32)
    packer = jnp.where(iota((slots, rows), 0) == slot, 1.0, 0.0).astype(BF16)
    mask = cell_mask(land[...], cols).astype(BF16)
    for c in range(CS):
        out[:, c * cols : (c + 1) * cols] = dot(packer, surface[c] * mask).astype(BF16)
    lanes = iota((rows, rows), 1)
    described = jnp.where(
        lanes == 0, across(weight[...]).T, jnp.where(lanes == 1, across(patch[...]).T, 0.0)
    )
    out[:, CS * cols :] = dot(packer, described.astype(BF16)).astype(BF16)


def common_kernel(turn, surface, out):
    side = surface.shape[1]
    k = turn[0, 0]
    flip_rows = reverser(side, k >= 2)
    flip_cols = reverser(side, (k == 1) | (k == 2))
    odd = (k % 2) == 1
    for c in range(CF):
        tile = surface[c].astype(F32)
        tile = jnp.where(odd, tile.T, tile).astype(BF16)
        tile = dot(tile, flip_cols).astype(BF16)
        out[:, c * side : (c + 1) * side] = dot(flip_rows, tile).astype(BF16)


def return_kernel(meta, rows, out):
    slots, side = meta.shape
    patch = meta[:, 1:2].astype(F32).astype(jnp.int32)
    select = jnp.where(iota((slots, side), 1) == patch, 1.0, 0.0).astype(BF16)
    for c in range(CF):
        part = slice(c * side, (c + 1) * side)
        out[:, part] = dot(select, rows[:, part]).astype(BF16)


def turn_edges(k, edges, size):
    width = edges[0].shape[1]
    rows, cols = iota((width, width), 0), iota((width, width), 1)
    flip = jnp.where(rows + cols == size - 1, 1.0, 0.0).astype(BF16)
    top, bottom, left, right = edges
    top_r, bottom_r, left_r, right_r = [dot(value.astype(BF16), flip) for value in edges]

    def chosen(*options):
        value = options[3]
        for number in range(3):
            value = jnp.where(k == number, options[number], value)
        return value

    return (
        chosen(top, left_r, bottom_r, right),
        chosen(bottom, right_r, top_r, left),
        chosen(left, bottom, right_r, top_r),
        chosen(right, top, left_r, bottom_r),
    )


def column_edges(ref):
    count, channels, cols = ref.shape
    lanes = iota((channels, count), 1)

    def step(y, carry):
        row = ref[y].astype(F32)
        return (
            jnp.where(lanes == y, row[:, 0:1], carry[0]),
            jnp.where(lanes == y, row[:, cols - 1 :], carry[1]),
        )

    zero = jnp.zeros((channels, count), F32)
    return lax.fori_loop(0, count, step, (zero, zero), unroll=16)


def all_edges(ref):
    last = ref.shape[0] - 1
    return (ref[0].astype(F32), ref[last].astype(F32), *column_edges(ref))


def early_kernel(turn, state, ocean, *outs):
    atmos = turn_edges(turn[0, 0], all_edges(state), state.shape[2])
    sea = all_edges(ocean)
    for out, above, below in zip(outs, atmos, sea):
        out[...] = jnp.concatenate([above, below], axis=0).astype(BF16)


def sea_kernel(turn, incoming, out, *edges):
    side = out.shape[0]
    slots = incoming.shape[0]
    k = turn[0, 0]
    flip_x = reverser(side, (k == 1) | (k == 2))
    meta = incoming[:, CS * side :].astype(F32)

    def placed(patch):
        patch = patch.astype(jnp.int32)
        return jnp.where(k >= 2, side - 1 - patch, patch)

    @pl.when((k % 2) == 0)
    def _():
        turned = meta.T
        spread = jnp.where(
            iota((side, slots), 0) == placed(turned[1:2, :]), turned[0:1, :], 0.0
        )
        scale = jnp.maximum(jnp.sum(spread, axis=1, keepdims=True), 1.0)
        spread = spread.astype(BF16)
        for c in range(CS):
            part = dot(incoming[:, c * side : (c + 1) * side], flip_x).astype(BF16)
            value = dot(spread, part) / scale
            out[:, c, :] = value.astype(BF16).astype(F32)

    @pl.when((k % 2) == 1)
    def _():
        spread = jnp.where(
            iota((slots, side), 1) == placed(meta[:, 1:2]), meta[:, 0:1], 0.0
        )
        scale = jnp.maximum(jnp.sum(spread, axis=0, keepdims=True), 1.0)
        spread = spread.astype(BF16)
        for c in range(CS):
            part = dot(incoming[:, c * side : (c + 1) * side], flip_x)
            value = dot(part.T.astype(BF16), spread) / scale
            out[:, c, :] = value.astype(BF16).astype(F32)

    for edge, value in zip(edges, turn_edges(k, all_edges(out), side)):
        edge[...] = value.astype(BF16)


def force_kernel(capacity, place, target, returned, out, *edges):
    rows, cols = out.shape[0], out.shape[2]
    slots = returned.shape[0]
    first, second = iota((rows, rows), 0), iota((rows, rows), 1)
    targets = across(target[...])
    same = (targets.T == targets) & (second < first)
    rank = jnp.sum(jnp.where(same, 1.0, 0.0), axis=1, keepdims=True)
    slot = (targets.T[:, 0:1] * capacity + rank).astype(jnp.int32)
    pick = jnp.where(iota((rows, slots), 1) == slot, 1.0, 0.0).astype(BF16)
    for c in range(CF):
        out[:, c, :] = dot(pick, returned[:, c * cols : (c + 1) * cols])
    for edge, value in zip(edges, paired(place, all_edges(out))):
        edge[...] = value.astype(BF16)


def paired(place, edges):
    first, last, left, right = edges
    even = place[0, 1] == 0
    return jnp.where(even, first, last), jnp.where(even, last, first), left, right


def widened(value):
    return jnp.concatenate([value, jnp.zeros_like(value)], axis=1)


def framed(before, value, after):
    cols = value.shape[1]
    lanes = iota((value.shape[0], 2 * cols), 1)
    moved = pltpu.roll(widened(value), 1, 1)
    return jnp.where(lanes == 0, before, jnp.where(lanes == cols + 1, after, moved))


def side_kernel(start, swaps, place, *refs):
    to_left, to_right, above_out, below_out = refs[-4:]
    left, right = refs[-6:-4]
    over, under = refs[0][...].astype(F32), refs[1][...].astype(F32)
    channels, cols = over.shape
    if swaps:
        even = place[0, 1] == 0
        over, under = jnp.where(even, over, under), jnp.where(even, under, over)
        back = dot(under.astype(BF16), reverser(cols, True))
        under = jnp.where(place[0, 0] == 1, back, under)
    elif start is not None:
        ocean = iota((channels, cols), 0) >= start
        over = jnp.where(ocean & (place[0, 0] == 0), 0.0, over)
        back = dot(refs[2][...], reverser(cols, True))
        back = jnp.concatenate([jnp.zeros((start, cols), F32), back], axis=0)
        under = jnp.where(ocean & (place[0, 0] == 1), back, under)
    above_out[...] = over.astype(BF16)
    below_out[...] = under.astype(BF16)
    to_left[...] = framed(over[:, :1], left[...].astype(F32), under[:, :1]).astype(BF16)
    to_right[...] = framed(
        over[:, cols - 1 :], right[...].astype(F32), under[:, cols - 1 :]
    ).astype(BF16)


def tap_kernel(splits, turn, *refs):
    count = len(splits)
    k = turn[0, 0]
    for number, (split, turned) in enumerate(splits):
        weight, out = refs[number], refs[count + number]
        outputs, channels = weight.shape[1:]
        for a in range(3):
            taps = []
            for b in range(3):
                at = 3 * a + b
                if turned:
                    moved = (3 * b + 2 - a, 8 - at, 3 * (2 - b) + a)
                    for quarter in range(3):
                        at = jnp.where(k == quarter + 1, moved[quarter], at)
                taps.append(weight[at].astype(F32))
            row = [tap[:, :split] for tap in taps]
            if split < channels:
                row += [tap[:, split:] for tap in taps]
            spare = out.shape[1] - 3 * channels
            if spare:
                row.append(jnp.zeros((outputs, spare), F32))
            out[a * outputs : (a + 1) * outputs, :] = jnp.concatenate(row, axis=1).astype(BF16)


def halo_kernel(spans, turned, turn, *refs):
    ends, left, right = refs[-3:]
    pieces = []
    for number, (low, high) in enumerate(spans):
        above, below, from_left, from_right = [
            ref[low:high, :].astype(F32) for ref in refs[4 * number : 4 * number + 4]
        ]
        last = above.shape[1] + 1
        pieces.append(
            (
                framed(from_left[:, :1], above, from_right[:, :1]),
                framed(from_left[:, last : last + 1], below, from_right[:, last : last + 1]),
                from_left,
                from_right,
            )
        )
    halo = [jnp.concatenate(part, axis=0) if len(part) > 1 else part[0] for part in zip(*pieces)]
    if turned:
        halo = turn_edges(lax.rem(4 - turn[0, 0], 4), halo, left.shape[1] + 2)
    ends[0], ends[1] = halo[0], halo[1]
    cols = left.shape[1]
    width = 2 * cols
    left[...] = pltpu.roll(halo[2], width - 1, 1)[:, :cols]
    right[...] = pltpu.roll(halo[3], width - 1, 1)[:, :cols]


def conv_kernel(parts, mode, *refs):
    refs = list(refs)
    turn = refs.pop(0)
    sources = [refs.pop(0) for _ in range(parts)]
    ends, left, right, taps = [refs.pop(0) for _ in range(4)]
    base = refs.pop(0) if mode in ("add", "masked") else None
    mask = refs.pop(0) if mode == "masked" else None
    out = refs.pop(0)
    gelu = mode in ("turned", "plain")
    edges = [refs.pop(0) for _ in range(4)] if gelu else None
    stacked, sums = refs[:2]
    edge_left, edge_right = refs[2:] if gelu else (None, None)
    rows, outputs, cols = out.shape
    channels = ends.shape[1]
    lanes = iota((channels, cols), 1)
    out_lanes = iota((outputs, cols), 1)

    spans, low = [], 0
    for source in sources:
        spans.append((low, low + source.shape[1]))
        low += source.shape[1]

    def place(slot, half, low, high, shifted):
        for b, value in enumerate(shifted):
            at = 3 * low + b * (high - low)
            stacked[slot, at : at + high - low, half * cols : (half + 1) * cols] = value.astype(
                BF16
            )

    def inner(slot, half, y):
        for source, (low, high) in zip(sources, spans):
            row = source[y].astype(F32)
            before = pltpu.roll(left[low:high, :], lax.rem(cols - y, cols), 1)
            after = pltpu.roll(right[low:high, :], cols - 1 - y, 1)
            shifts = (
                jnp.where(lanes[low:high] == 0, before, pltpu.roll(row, 1, 1)),
                row,
                jnp.where(lanes[low:high] == cols - 1, after, pltpu.roll(row, cols - 1, 1)),
            )
            place(slot, half, low, high, shifts)

    def end(slot, half, which):
        for low, high in spans:
            row = ends[which, low:high, :]
            place(slot, half, low, high, [row[:, b : b + cols] for b in range(3)])

    def emit(y, value):
        if gelu:
            value = jax.nn.gelu(value, approximate=True).astype(BF16)
            out[y] = value
            return value.astype(F32)
        value = base[y].astype(F32) + value
        if mode == "masked":
            value = value * mask[y]
        out[y] = value.astype(BF16)
        return None

    def product(slot):
        sums[slot] = dot(taps[...], stacked[slot])

    def tap(slot, a, half):
        return sums[slot, a * outputs : (a + 1) * outputs, half * cols : (half + 1) * cols]

    def finish(slot, j):
        was = (slot + 3) % 4
        rows_of = [
            (2 * j - 2, tap(was, 0, 0) + tap(was, 1, 1) + tap(slot, 2, 0)),
            (2 * j - 1, tap(was, 0, 1) + tap(slot, 1, 0) + tap(slot, 2, 1)),
        ]
        return [(y, emit(y, value)) for y, value in rows_of]

    def note(done):
        if gelu:
            first, last = edge_left[...], edge_right[...]
            for y, value in done:
                first = jnp.where(out_lanes == y, value[:, 0:1], first)
                last = jnp.where(out_lanes == y, value[:, cols - 1 :], last)
            edge_left[...] = first
            edge_right[...] = last

    def load(slot, j):
        inner(slot, 0, 2 * j - 1)
        inner(slot, 1, 2 * j)

    spare = stacked.shape[1] - 3 * channels
    if spare:
        stacked[:, 3 * channels :, :] = jnp.zeros((stacked.shape[0], spare, 2 * cols), BF16)
    if gelu:
        edge_left[...] = jnp.zeros(edge_left.shape, F32)
        edge_right[...] = jnp.zeros(edge_right.shape, F32)
    pairs = rows // 2
    assert pairs % 4 == 0 and pairs >= 8
    end(3, 0, 0)
    inner(3, 1, 0)
    load(0, 1)
    load(1, 2)
    product(3)
    product(0)
    product(1)
    load(2, 3)
    load(3, 4)

    def half(j, now, other, final=False):
        product(now)
        done = finish(other, j - 2)
        load(other, j + 2)
        product(now + 1)
        done += finish(other + 1, j - 1)
        if final:
            inner(other + 1, 0, rows - 1)
            end(other + 1, 1, 1)
        else:
            load(other + 1, j + 3)
        note(done)

    def step(i, _):
        half(4 * i + 3, 2, 0)
        half(4 * i + 5, 0, 2)
        return 0

    lax.fori_loop(0, (pairs - 8) // 4, step, 0)
    half(pairs - 5, 2, 0)
    half(pairs - 3, 0, 2, True)
    product(2)
    done = finish(0, pairs - 3)
    product(3)
    done += finish(1, pairs - 2)
    note(done)
    note(finish(2, pairs - 1) + finish(3, pairs))
    if gelu:
        found = (
            out[0].astype(F32),
            out[rows - 1].astype(F32),
            edge_left[...],
            edge_right[...],
        )
        if mode == "turned":
            found = turn_edges(turn[0, 0], found, cols)
        else:
            found = paired(turn, found)
        for edge, value in zip(edges, found):
            edge[...] = value.astype(BF16)


def convolve(turn, sources, halo, taps, mode, base=None, mask=None):
    rows, _, cols = sources[0].shape
    outputs = taps.shape[0] // 3
    operands = [turn, *sources, *halo, taps]
    operands += [value for value in (base, mask) if value is not None]
    shapes = [jax.ShapeDtypeStruct((rows, outputs, cols), BF16)]
    scratch = [
        pltpu.VMEM((4, taps.shape[1], 2 * cols), BF16),
        pltpu.VMEM((4, taps.shape[0], 2 * cols), F32),
    ]
    if base is None:
        shapes += [jax.ShapeDtypeStruct((outputs, cols), BF16)] * 4
        scratch += [pltpu.VMEM((outputs, cols), F32)] * 2
    result = pl.pallas_call(
        partial(conv_kernel, len(sources), mode),
        out_shape=shapes,
        in_specs=[SM] + [VM] * (len(operands) - 1),
        out_specs=[VM] * len(shapes),
        scratch_shapes=scratch,
        cost_estimate=lasting(rows * outputs * taps.shape[1] / 700000),
        compiler_params=SMALL,
    )(*operands)
    return (result[0], result[1:]) if base is None else result[0]


def spans_of(sources):
    spans, low = [], 0
    for source in sources:
        spans.append((low, low + source.shape[1]))
        low += source.shape[1]
    return spans


def main_kernel(parts, mode, *refs):
    refs = list(refs)
    sources = [refs.pop(0) for _ in range(parts)]
    taps = refs.pop(0)
    base = refs.pop(0) if mode != "gelu" else None
    mask = refs.pop(0) if mode == "masked" else None
    out, edge_left, edge_right, stacked, sums = refs
    rows, outputs, cols = out.shape
    spans = spans_of(sources)
    channels = spans[-1][1]
    lanes = iota((channels, cols), 1)
    out_lanes = iota((outputs, cols), 1)

    def place(slot, half, low, high, shifted):
        for b, value in enumerate(shifted):
            at = 3 * low + b * (high - low)
            stacked[slot, at : at + high - low, half * cols : (half + 1) * cols] = value.astype(
                BF16
            )

    def inner(slot, half, y):
        for source, (low, high) in zip(sources, spans):
            row = source[y].astype(F32)
            shifts = (
                jnp.where(lanes[low:high] == 0, 0.0, pltpu.roll(row, 1, 1)),
                row,
                jnp.where(lanes[low:high] == cols - 1, 0.0, pltpu.roll(row, cols - 1, 1)),
            )
            place(slot, half, low, high, shifts)

    def end(slot, half):
        for low, high in spans:
            place(slot, half, low, high, [jnp.zeros((high - low, cols), F32)] * 3)

    def emit(y, value):
        result = value
        if mode == "gelu":
            result = jax.nn.gelu(value, approximate=True)
        else:
            result = base[y].astype(F32) + value
            if mode == "masked":
                result = result * mask[y]
        out[y] = result.astype(BF16)
        return value

    def product(slot):
        sums[slot] = dot(taps[...], stacked[slot])

    def tap(slot, a, half):
        return sums[slot, a * outputs : (a + 1) * outputs, half * cols : (half + 1) * cols]

    def finish(slot, j):
        was = (slot + 3) % 4
        rows_of = [
            (2 * j - 2, tap(was, 0, 0) + tap(was, 1, 1) + tap(slot, 2, 0)),
            (2 * j - 1, tap(was, 0, 1) + tap(slot, 1, 0) + tap(slot, 2, 1)),
        ]
        return [(y, emit(y, value)) for y, value in rows_of]

    def note(done):
        first, last = edge_left[...], edge_right[...]
        for y, value in done:
            first = jnp.where(out_lanes == y, value[:, 0:1], first)
            last = jnp.where(out_lanes == y, value[:, cols - 1 :], last)
        edge_left[...] = first
        edge_right[...] = last

    def load(slot, j):
        inner(slot, 0, 2 * j - 1)
        inner(slot, 1, 2 * j)

    spare = stacked.shape[1] - 3 * channels
    if spare:
        stacked[:, 3 * channels :, :] = jnp.zeros((stacked.shape[0], spare, 2 * cols), BF16)
    edge_left[...] = jnp.zeros(edge_left.shape, F32)
    edge_right[...] = jnp.zeros(edge_right.shape, F32)
    pairs = rows // 2
    assert pairs % 4 == 0 and pairs >= 8
    end(3, 0)
    inner(3, 1, 0)
    load(0, 1)
    load(1, 2)
    product(3)
    product(0)
    product(1)
    load(2, 3)
    load(3, 4)

    def half(j, now, other, final=False):
        product(now)
        done = finish(other, j - 2)
        load(other, j + 2)
        product(now + 1)
        done += finish(other + 1, j - 1)
        if final:
            inner(other + 1, 0, rows - 1)
            end(other + 1, 1)
        else:
            load(other + 1, j + 3)
        note(done)

    def step(i, _):
        half(4 * i + 3, 2, 0)
        half(4 * i + 5, 0, 2)
        return 0

    lax.fori_loop(0, (pairs - 8) // 4, step, 0)
    half(pairs - 5, 2, 0)
    half(pairs - 3, 0, 2, True)
    product(2)
    done = finish(0, pairs - 3)
    product(3)
    done += finish(1, pairs - 2)
    note(done)
    note(finish(2, pairs - 1) + finish(3, pairs))


def convolve_alone(sources, taps, mode, base=None, mask=None):
    rows, _, cols = sources[0].shape
    outputs = taps.shape[0] // 3
    operands = [*sources, taps]
    operands += [value for value in (base, mask) if value is not None]
    return pl.pallas_call(
        partial(main_kernel, len(sources), mode),
        out_shape=[jax.ShapeDtypeStruct((rows, outputs, cols), BF16)]
        + [jax.ShapeDtypeStruct((outputs, rows), F32)] * 2,
        in_specs=[VM] * len(operands),
        out_specs=[VM] * 3,
        scratch_shapes=[
            pltpu.VMEM((4, taps.shape[1], 2 * cols), BF16),
            pltpu.VMEM((4, taps.shape[0], 2 * cols), F32),
        ],
        cost_estimate=lasting(rows * outputs * taps.shape[1] / 700000),
        compiler_params=SMALL,
    )(*operands)


def edge_kernel(parts, mode, where, *refs):
    refs = list(refs)
    main, side_left, side_right = [refs.pop(0) for _ in range(3)]
    sources = [refs.pop(0) for _ in range(2 * parts)]
    ends, left, right, taps = [refs.pop(0) for _ in range(4)]
    base = refs.pop(0) if mode in ("add", "masked") else None
    mask = refs.pop(0) if mode == "masked" else None
    gelu = mode in ("turned", "plain")
    out = refs.pop(0)
    edges = [refs.pop(0) for _ in range(4)] if gelu else None
    stacked = refs.pop(0)
    rows, outputs, cols = out.shape
    spans = spans_of(sources[:parts])
    channels = spans[-1][1]
    lanes = iota((channels, cols), 1)
    out_lanes = iota((outputs, cols), 1)
    if stacked.shape[1] > 3 * channels:
        spare = stacked.shape[1] - 3 * channels
        stacked[:, 3 * channels :, :] = jnp.zeros((stacked.shape[0], spare, 2 * cols), BF16)

    def place(slot, half, low, high, shifted):
        for b, value in enumerate(shifted):
            at = 3 * low + b * (high - low)
            stacked[slot, at : at + high - low, half * cols : (half + 1) * cols] = value.astype(
                BF16
            )

    def end(slot, half, which):
        for low, high in spans:
            row = ends[which, low:high, :]
            place(slot, half, low, high, [row[:, b : b + cols] for b in range(3)])

    def inner(slot, half, late, at):
        for number, (low, high) in enumerate(spans):
            row = sources[number + parts * late][at].astype(F32)
            y = (rows - 2) * late + at
            before = pltpu.roll(left[low:high, :], (cols - y) % cols, 1)
            after = pltpu.roll(right[low:high, :], cols - 1 - y, 1)
            shifts = (
                jnp.where(lanes[low:high] == 0, before, pltpu.roll(row, 1, 1)),
                row,
                jnp.where(lanes[low:high] == cols - 1, after, pltpu.roll(row, cols - 1, 1)),
            )
            place(slot, half, low, high, shifts)

    end(0, 0, 0)
    inner(1, 0, 0, 0)
    inner(2, 0, 0, 1)
    inner(0, 1, 1, 0)
    inner(1, 1, 1, 1)
    end(2, 1, 1)
    for a, distance in enumerate((1, 0, cols - 1)):
        for low, high in spans:
            zero = jnp.zeros((high - low, cols), F32)
            before, after = left[low:high, :], right[low:high, :]
            if distance:
                before, after = pltpu.roll(before, distance, 1), pltpu.roll(after, distance, 1)
            place(3 + a, 0, low, high, (before, zero, zero))
            place(3 + a, 1, low, high, (zero, zero, after))

    def product(slot):
        a = slot % 3
        return dot(taps[a * outputs : (a + 1) * outputs, :], stacked[slot])

    ended = product(0) + product(1) + product(2)
    sided = product(3) + product(4) + product(5)
    top, bottom = ended[:, :cols], ended[:, cols:]
    first = side_left[...] + sided[:, :cols]
    last = side_right[...] + sided[:, cols:]
    if gelu:
        top, bottom, first, last = [
            jax.nn.gelu(value, approximate=True).astype(BF16).astype(F32)
            for value in (top, bottom, first, last)
        ]

    def complete(y, value):
        if gelu:
            return value
        value = base[y].astype(F32) + value
        return value * mask[y] if mode == "masked" else value

    def step(y, _):
        before = pltpu.roll(first, lax.rem(cols - y, cols), 1)
        after = pltpu.roll(last, cols - 1 - y, 1)
        side = complete(y, jnp.where(out_lanes == 0, before, after))
        inside = (out_lanes > 0) & (out_lanes < cols - 1)
        out[y] = jnp.where(inside, main[y].astype(F32), side).astype(BF16)
        return 0

    lax.fori_loop(0, rows, step, 0, unroll=8)
    out[0] = complete(0, top).astype(BF16)
    out[rows - 1] = complete(rows - 1, bottom).astype(BF16)
    if gelu:

        def ended_column(value, at):
            value = jnp.where(out_lanes == 0, top[:, at : at + 1], value)
            return jnp.where(out_lanes == rows - 1, bottom[:, at : at + 1], value)

        found = (top, bottom, ended_column(first, 0), ended_column(last, cols - 1))
        if mode == "turned":
            found = turn_edges(where[0, 0], found, cols)
        else:
            found = paired(where, found)
        for edge, value in zip(edges, found):
            edge[...] = value.astype(BF16)


def with_edges(where, main, sources, halo, taps, mode, base=None, mask=None):
    rows, outputs, cols = main[0].shape
    pairs = rows // 2

    def pair_of(values, number):
        return pl.BlockSpec((2, *values.shape[1:]), lambda i: (number, 0, 0))

    operands = [*main, *sources, *sources, *halo, taps]
    extra = [value for value in (base, mask) if value is not None]
    specs = [VM] * 3
    specs += [pair_of(value, 0) for value in sources]
    specs += [pair_of(value, pairs - 1) for value in sources]
    specs += [VM] * (len(halo) + 1 + len(extra))
    shapes = [jax.ShapeDtypeStruct((rows, outputs, cols), BF16)]
    if base is None:
        shapes += [jax.ShapeDtypeStruct((outputs, cols), BF16)] * 4
    result = pl.pallas_call(
        partial(edge_kernel, len(sources), mode),
        grid=(1,),
        out_shape=shapes,
        in_specs=[SM] + specs,
        out_specs=[VM] * len(shapes),
        scratch_shapes=[pltpu.VMEM((6, taps.shape[1], 2 * cols), BF16)],
        cost_estimate=lasting(3),
        compiler_params=SMALL,
    )(where, *operands, *extra)
    return (result[0], result[1:]) if base is None else result[0]


def shifted(value, axis, distance):
    count = lax.axis_size(axis)
    return lax.ppermute(value, axis, [(i, (i + distance) % count) for i in range(count)])


def send_rows(edges, start=None, swaps=False):
    top, bottom = edges[:2]
    faces, tiles = lax.axis_size("face"), lax.axis_size("tile")
    north = (faces - 1) * tiles
    axes = ("face", "tile")
    fold = [(north + t, north + tiles - 1 - t) for t in range(tiles)]
    if swaps:
        assert faces % 2 == 0

        def swap(low):
            return [
                (source * tiles + t, target * tiles + t)
                for at in range(low, faces - 1, 2)
                for source, target in ((at, at + 1), (at + 1, at))
                for t in range(tiles)
            ]

        return [lax.ppermute(top, axes, swap(1) + fold), lax.ppermute(bottom, axes, swap(0))]
    rows = [shifted(bottom, "face", 1), shifted(top, "face", -1)]
    if start is not None:
        rows.append(lax.ppermute(bottom[start:], axes, fold))
    return rows


def sides_of(place, rows, edges, start=None, swaps=False):
    operands = [*rows, *edges[2:]]
    channels, cols = edges[0].shape
    return pl.pallas_call(
        partial(side_kernel, start, swaps),
        out_shape=[jax.ShapeDtypeStruct((channels, 2 * cols), BF16)] * 2
        + [jax.ShapeDtypeStruct((channels, cols), BF16)] * 2,
        in_specs=[SM] + [VM] * len(operands),
        out_specs=[VM] * 4,
        cost_estimate=lasting(1),
        compiler_params=SMALL,
    )(place, *operands)


def send_sides(sides):
    to_left, to_right, above, below = sides
    return above, below, shifted(to_right, "tile", 1), shifted(to_left, "tile", -1)


def exchanged(edges, place, **how):
    return send_sides(sides_of(place, send_rows(edges, **how), edges, **how))


def halo_of(turn, spans, turned, *pieces):
    channels = sum(high - low for low, high in spans)
    cols = pieces[0][0].shape[1]
    operands = [value for piece in pieces for value in piece]
    return pl.pallas_call(
        partial(halo_kernel, spans, turned),
        out_shape=[jax.ShapeDtypeStruct((2, channels, 2 * cols), F32)]
        + [jax.ShapeDtypeStruct((channels, cols), F32)] * 2,
        in_specs=[SM] + [VM] * len(operands),
        out_specs=[VM] * 3,
        cost_estimate=lasting(1),
        compiler_params=SMALL,
    )(turn, *operands)


def stack_taps(turn, weights, splits):
    def shape(weight):
        _, outputs, channels = weight.shape
        wide = 3 * channels + -3 * channels % 128
        return jax.ShapeDtypeStruct((3 * outputs, wide), BF16)

    return pl.pallas_call(
        partial(tap_kernel, splits),
        out_shape=[shape(weight) for weight in weights],
        in_specs=[SM] + [VM] * len(weights),
        out_specs=[VM] * len(weights),
        cost_estimate=lasting(1),
        compiler_params=SMALL,
    )(turn, *weights)


def on_device(
    atmos_state,
    ocean_state,
    land_mask,
    face_turns,
    block_target,
    block_patch,
    block_weight,
    atmos_w1,
    atmos_w2,
    ocean_w1,
    ocean_w2,
):
    state_channels, side = atmos_state.shape[0], atmos_state.shape[2]
    ocean_channels, rows, cols = ocean_state.shape
    devices = lax.axis_size(("face", "tile"))
    capacity = max(2, 2 * rows // devices)
    slots = devices * capacity
    axes = ("face", "tile")
    face = lax.axis_index("face")
    end = jnp.where(face == 0, 0, jnp.where(face == lax.axis_size("face") - 1, 1, 2))
    place = jnp.stack([end, face % 2]).astype(jnp.int32).reshape(1, 2)

    def surface_spec(values, channels):
        return pl.BlockSpec((channels, *values.shape[1:]), lambda i: (0, 0, 0))

    def whole(values):
        return pl.BlockSpec(values.shape, lambda i: (0,) * values.ndim)

    def edge_shapes(channels):
        return [jax.ShapeDtypeStruct((channels, cols), BF16)] * 4

    target = block_target.reshape(1, rows)
    small = (land_mask.T, target, block_weight.reshape(1, rows), block_patch.reshape(1, rows))
    payload = pl.pallas_call(
        partial(pack_kernel, capacity),
        grid=(1,),
        out_shape=jax.ShapeDtypeStruct((slots, (CS + 1) * cols), BF16),
        in_specs=[surface_spec(ocean_state, CS)] + [whole(values) for values in small],
        out_specs=VM,
        cost_estimate=lasting(1),
        compiler_params=SMALL,
    )(ocean_state, *small)
    incoming = lax.all_to_all(payload, axes, split_axis=0, concat_axis=0, tiled=True)

    state = atmos_state.transpose(1, 0, 2)
    mask = jnp.repeat(land_mask, RUN, axis=1).astype(BF16)
    ocean = (ocean_state * mask[None]).transpose(1, 0, 2)
    early = pl.pallas_call(
        early_kernel,
        out_shape=edge_shapes(state_channels + ocean_channels),
        in_specs=[SM, VM, VM],
        out_specs=[VM] * 4,
        cost_estimate=lasting(6),
        compiler_params=SMALL,
    )(face_turns, state, ocean)
    early_halo = exchanged(early, place, start=state_channels)

    taps1, taps2, ocean_taps1, ocean_taps2 = stack_taps(
        face_turns,
        (atmos_w1, atmos_w2, ocean_w1, ocean_w2),
        (
            (state_channels, True),
            (state_channels, True),
            (ocean_channels, False),
            (ocean_channels, False),
        ),
    )
    common_rows = pl.pallas_call(
        common_kernel,
        grid=(1,),
        out_shape=jax.ShapeDtypeStruct((side, CF * side), BF16),
        in_specs=[SM, surface_spec(atmos_state, CF)],
        out_specs=VM,
        cost_estimate=lasting(1),
        compiler_params=SMALL,
    )(face_turns, atmos_state)
    incoming, state, ocean, early_halo, common_rows, taps1, taps2, ocean_taps1, ocean_taps2 = (
        lax.optimization_barrier(
            (
                incoming,
                state,
                ocean,
                early_halo,
                common_rows,
                taps1,
                taps2,
                ocean_taps1,
                ocean_taps2,
            )
        )
    )
    answer = pl.pallas_call(
        return_kernel,
        grid=(1,),
        out_shape=jax.ShapeDtypeStruct((slots, CF * side), BF16),
        in_specs=[pl.BlockSpec((slots, side), lambda i: (0, CS)), VM],
        out_specs=VM,
        cost_estimate=lasting(1),
        compiler_params=SMALL,
    )(incoming, common_rows)

    barrier = lax.optimization_barrier
    incoming, answer = barrier((incoming, answer))
    returned = lax.all_to_all(answer, axes, split_axis=0, concat_axis=0, tiled=True)
    sea, *sea_edges = pl.pallas_call(
        sea_kernel,
        out_shape=[jax.ShapeDtypeStruct((side, CS, side), F32), *edge_shapes(CS)],
        in_specs=[SM, VM],
        out_specs=[VM] * 5,
        cost_estimate=lasting(3),
        compiler_params=SMALL,
    )(face_turns, incoming)
    sea_rows = send_rows(sea_edges)
    hidden_main = convolve_alone([state, sea], taps1, "gelu")
    sea_rows, hidden_main = barrier((sea_rows, hidden_main))
    sea_halo = send_sides(sides_of(place, sea_rows, sea_edges))
    forcing, *forcing_edges = pl.pallas_call(
        partial(force_kernel, capacity),
        out_shape=[jax.ShapeDtypeStruct((rows, CF, cols), F32), *edge_shapes(CF)],
        in_specs=[SM, VM, VM],
        out_specs=[VM] * 5,
        cost_estimate=lasting(3),
        compiler_params=SMALL,
    )(place, target, returned)
    forcing_rows = send_rows(forcing_edges, swaps=True)

    state_span = (0, state_channels)
    sea_halo, _ = barrier((sea_halo, forcing))
    halo = halo_of(face_turns, [state_span, (0, CS)], True, early_halo, sea_halo)
    hidden, hidden_edges = with_edges(
        face_turns, hidden_main, [state, sea], halo, taps1, "turned"
    )
    forcing_rows, hidden_edges = barrier((forcing_rows, hidden_edges))
    forcing_sides = sides_of(place, forcing_rows, forcing_edges, swaps=True)
    forcing_halo = send_sides(forcing_sides)
    hidden_sides = sides_of(place, send_rows(hidden_edges), hidden_edges)
    hidden_halo = send_sides(hidden_sides)

    ocean_span = (state_channels, state_channels + ocean_channels)
    forcing, _ = barrier((forcing, hidden_sides[0]))
    halo = halo_of(face_turns, [ocean_span, (0, CF)], False, early_halo, forcing_halo)
    hidden_ocean, ocean_edges = convolve(place, [ocean, forcing], halo, ocean_taps1, "plain")

    ocean_sent = send_rows(ocean_edges, swaps=True)
    halo = halo_of(face_turns, [state_span], True, hidden_halo)
    hidden, _ = barrier((hidden, hidden_ocean))
    atmos_out = convolve(face_turns, [hidden], halo, taps2, "add", base=state)
    ocean_sent, atmos_out = barrier((ocean_sent, atmos_out))
    ocean_halo = send_sides(sides_of(place, ocean_sent, ocean_edges, swaps=True))
    atmos_out = with_layout_constraint(atmos_out.transpose(1, 0, 2), Layout((0, 1, 2)))
    ocean_halo, atmos_out = barrier((ocean_halo, atmos_out))
    halo = halo_of(face_turns, [(0, ocean_channels)], False, ocean_halo)
    ocean_out = convolve(
        place,
        [hidden_ocean],
        halo,
        ocean_taps2,
        "masked",
        base=ocean,
        mask=mask.astype(F32)[:, None, :],
    )
    return atmos_out, ocean_out.transpose(1, 0, 2)


def solution(mesh):
    placed = (
        P(None, "face", "tile"),
        P(None, "face", "tile"),
        P("face", "tile"),
        P("face", "tile"),
        P(("face", "tile"), None),
        P(("face", "tile"), None),
        P(("face", "tile"), None),
        P(),
        P(),
        P(),
        P(),
    )
    return jax.shard_map(
        on_device,
        mesh=mesh,
        in_specs=placed,
        out_specs=(P(None, "face", "tile"), P(None, "face", "tile")),
        check_vma=False,
    )
```
